32 devices in a mesh: rep: 1 (over z), vocab: 32 (over y, x, core).
Axes of the slice: x: 4, y: 4, z: 1, core: 2. Of those that a mesh axis runs over, the one named last changes fastest.
The devices are a block of a 4x4x8 slice.
Arguments:
- hidden: bfloat16 [16384, 4096], P(('rep', 'vocab'))
- w_head: bfloat16 [32768, 4096], P('vocab')
- allowed_ids: int32 [2048], P('rep')
- allowed_valid: int32 [2048], P('rep')
- target_pos: int32 [16384], P(('rep', 'vocab'))
Outputs:
- output 1: float32 [16384, 2048], P(('rep', 'vocab'))
- output 2: float32 [16384], P(('rep', 'vocab'))
All inputs are finite; a program needn't handle non-finite values.
Results may differ from the reference program's by a relative error of at most 0.001.
Values are sent between devices in bfloat16 or wider.
A program may use at most 768 MiB of HBM per device.

```python
import jax
import jax.numpy as jnp
from jax import lax

VOCAB_SIZE = 32768
MODEL_DIM = 4096
LIST_LEN = 2048
BATCH_ROWS = 16384
SHARDS = 32
HEAD_BLOCKS = 128
INV_TEMP = 1.25


def draw_head(key_head):
    block_keys = jax.random.split(key_head, HEAD_BLOCKS)
    row_scale = MODEL_DIM ** -0.5

    def one_block(block_key):
        block_vals = jax.random.normal(block_key, (VOCAB_SIZE // HEAD_BLOCKS, MODEL_DIM), jnp.float32)
        return (block_vals * row_scale).astype(jnp.bfloat16)

    return lax.map(one_block, block_keys).reshape(VOCAB_SIZE, MODEL_DIM)


def draw_list(key_list):
    key_pair, key_move, key_offset, key_order, key_count, key_valid, key_target = jax.random.split(key_list, 7)
    per_shard = LIST_LEN // SHARDS
    slot_cap = 2 * per_shard
    vocab_local = VOCAB_SIZE // SHARDS
    shard_order = jax.random.permutation(key_pair, SHARDS)
    move_sizes = jax.random.randint(key_move, (SHARDS // 2,), 0, per_shard + 1).at[0].set(per_shard)
    shard_gain = jnp.zeros((SHARDS,), jnp.int32).at[shard_order[0::2]].set(move_sizes).at[shard_order[1::2]].set(-move_sizes)
    counts = per_shard + shard_gain
    offset_keys = jax.random.split(key_offset, SHARDS)
    offsets = jax.vmap(lambda one_key: jax.random.permutation(one_key, vocab_local)[:slot_cap])(offset_keys)
    candidates = jnp.arange(SHARDS, dtype=jnp.int32)[:, None] * vocab_local + offsets
    keep_slot = jnp.arange(slot_cap)[None, :] < counts[:, None]
    sort_key = jnp.where(keep_slot, 0, 1) * (SHARDS * slot_cap) + jnp.arange(SHARDS * slot_cap).reshape(SHARDS, slot_cap)
    chosen = jnp.argsort(sort_key.reshape(-1))[:LIST_LEN]
    grouped = candidates.reshape(-1)[chosen]
    allowed_ids = grouped[jax.random.permutation(key_order, LIST_LEN)].astype(jnp.int32)
    valid_count = jax.random.randint(key_count, (), LIST_LEN // 2, LIST_LEN + 1)
    valid_perm = jax.random.permutation(key_valid, LIST_LEN)
    allowed_valid = (valid_perm < valid_count).astype(jnp.int32)
    inverse = jnp.argsort(valid_perm)
    pick_rank = jax.random.randint(key_target, (BATCH_ROWS,), 0, valid_count)
    target_pos = inverse[pick_rank].astype(jnp.int32)
    return allowed_ids, allowed_valid, target_pos


def setup_inputs(seed: int = 0, part: int = 0) -> dict:
    root_key = jax.random.key(seed)
    key_head, key_groups = jax.random.split(root_key)
    key_part = jax.random.fold_in(key_groups, part)
    key_hidden, key_list = jax.random.split(key_part)
    hidden = jax.random.normal(key_hidden, (BATCH_ROWS, MODEL_DIM), jnp.float32).astype(jnp.bfloat16)
    allowed_ids, allowed_valid, target_pos = draw_list(key_list)
    return dict(hidden=hidden, w_head=draw_head(key_head), allowed_ids=allowed_ids, allowed_valid=allowed_valid, target_pos=target_pos)


def reference(hidden, w_head, allowed_ids, allowed_valid, target_pos):
    head_rows = jnp.take(w_head, allowed_ids, axis=0)
    scores = jnp.dot(hidden, head_rows.T, preferred_element_type=jnp.float32) * INV_TEMP
    keep_mask = (allowed_valid > 0)[None, :]
    masked = jnp.where(keep_mask, scores, -jnp.inf)
    log_norm = jax.nn.logsumexp(masked, axis=1)
    token_probs = jnp.where(keep_mask, jnp.exp(masked - log_norm[:, None]), 0.0)
    picked = jnp.take_along_axis(scores, target_pos[:, None], axis=1)[:, 0]
    return token_probs, picked - log_norm
```

```python
import jax
import jax.numpy as jnp
from jax import lax
from jax.sharding import PartitionSpec as P

INV_TEMP = 1.25


def ranks(owner, shards):
    n = owner.shape[0]
    block = 128
    hot = (owner[:, None] == jnp.arange(shards)[None, :]).astype(jnp.bfloat16).reshape(n // block, block, shards)
    below = (jnp.arange(block)[:, None] > jnp.arange(block)[None, :]).astype(jnp.bfloat16)
    inside = jnp.einsum('ij,bjs->bis', below, hot, preferred_element_type=jnp.float32)
    totals = jnp.sum(hot.astype(jnp.float32), axis=1)
    nb = n // block
    before = jnp.sum(jnp.where((jnp.arange(nb)[:, None] > jnp.arange(nb)[None, :])[:, :, None], totals[None], 0.0), axis=1)
    rank = jnp.sum((inside + before[:, None, :]) * hot.astype(jnp.float32), axis=2).reshape(n)
    return rank.astype(jnp.int32), jnp.sum(totals, axis=0).astype(jnp.int32)


def solution(mesh):
    shards = mesh.shape['vocab']

    def device_step(hidden, w_head, allowed_ids, allowed_valid, target_pos):
        me = lax.axis_index('vocab')
        vocab_local, depth = w_head.shape
        n = allowed_ids.shape[0]
        cap = 2 * n // shards
        cols = depth // shards
        owner = allowed_ids // vocab_local
        rank, counts = ranks(owner, shards)
        rounds = (jnp.max(counts) + cap - 1) // cap

        def exchange(i):
            slot = rank - i * cap
            mine = (owner == me)[None, :] & (slot[None, :] == jnp.arange(cap)[:, None])
            local = jnp.sum(jnp.where(mine, (allowed_ids - me * vocab_local)[None, :] + 1, 0), axis=1) - 1
            pick = (local[:, None] == jnp.arange(vocab_local)[None, :]).astype(jnp.bfloat16)
            rows = jnp.dot(pick, w_head, preferred_element_type=jnp.float32).astype(jnp.bfloat16)
            out = rows.reshape(cap, shards, cols).transpose(1, 0, 2)
            got = lax.all_to_all(out, 'vocab', 0, 0).reshape(shards * cap, cols)
            code = jnp.where((slot >= 0) & (slot < cap), owner * cap + slot, -1)
            place = (code[:, None] == jnp.arange(shards * cap)[None, :]).astype(jnp.bfloat16)
            return jnp.dot(place, got, preferred_element_type=jnp.float32).astype(jnp.bfloat16)

        slices = lax.fori_loop(1, rounds, lambda i, acc: acc + exchange(i), exchange(0))
        every = lax.all_gather(slices, 'vocab', axis=0)
        scores = jnp.einsum('bdk,djk->bj', hidden.reshape(hidden.shape[0], shards, cols), every, preferred_element_type=jnp.float32) * INV_TEMP
        keep = (allowed_valid > 0)[None, :]
        masked = jnp.where(keep, scores, -jnp.inf)
        log_norm = jax.nn.logsumexp(masked, axis=1)
        probs = jnp.where(keep, jnp.exp(masked - log_norm[:, None]), 0.0)
        hit = target_pos[:, None] == jnp.arange(n)[None, :]
        picked = jnp.sum(jnp.where(hit, scores, 0.0), axis=1)
        return probs, picked - log_norm

    row_spec = P(('rep', 'vocab'))
    mat_spec = P(('rep', 'vocab'), None)
    return jax.shard_map(device_step, mesh=mesh, in_specs=(mat_spec, P('vocab', None), P('rep'), P('rep'), row_spec), out_specs=(mat_spec, row_spec), check_vma=False)
```

```python
import functools
import math

import jax
import jax.numpy as jnp
from jax import lax
from jax.experimental import pallas as pl
from jax.experimental.pallas import tpu as pltpu
from jax.sharding import PartitionSpec as P

INV_TEMP = 1.25
F32, BF16, I32 = jnp.float32, jnp.bfloat16, jnp.int32


def ranks(owner, shards):
    n = owner.shape[0]
    block = 128
    hot = (owner[:, None] == jnp.arange(shards)[None, :]).astype(BF16).reshape(n // block, block, shards)
    below = (jnp.arange(block)[:, None] > jnp.arange(block)[None, :]).astype(BF16)
    inside = jnp.einsum('ij,bjs->bis', below, hot, preferred_element_type=F32)
    totals = jnp.sum(hot.astype(F32), axis=1)
    nb = n // block
    before = jnp.sum(jnp.where((jnp.arange(nb)[:, None] > jnp.arange(nb)[None, :])[:, :, None], totals[None], 0.0), axis=1)
    rank = jnp.sum((inside + before[:, None, :]) * hot.astype(F32), axis=2).reshape(n)
    return rank.astype(I32), jnp.sum(totals, axis=0).astype(I32)


def gather_kernel(side, cap, hid_hbm, head_hbm, pick_ref, code_ref, out_hbm,
                  hid, head, pick, made, got, part, gat, acc,
                  hid_sem, head_sem, made_sem, got_sem, ring_send, ring_recv, pair_send, pair_recv, out_sem):
    chips = side * side
    devs = 2 * chips
    cols = made.shape[2]
    listed = gat.shape[1]
    half = listed // 2
    me = lax.axis_index('vocab')
    core = lax.rem(me, 2)
    chip = me // 2
    x, y = lax.rem(chip, side), chip // side

    def dev(a, b, c):
        px = lax.rem(x + a * (1 - c) + b * c, side)
        py = lax.rem(y + a * c + b * (1 - c), side)
        return (py * side + px) * 2 + c

    barrier = pltpu.get_barrier_semaphore()

    def greet(i, _):
        pl.semaphore_signal(barrier, inc=1, device_id={'vocab': lax.rem(me + i, devs)}, device_id_type=pl.DeviceIdType.MESH)
        return 0

    def turn(i):
        return lax.rem(chip + 1 + i, chips)

    def head_copy(q):
        return pltpu.make_async_copy(head_hbm.at[:, pl.ds(pl.multiple_of(q * 2 * cols, 2 * cols), 2 * cols)], head.at[q], head_sem.at[q])

    def head_start(i, _):
        head_copy(turn(i)).start()
        return 0

    lax.fori_loop(0, chips, head_start, 0)
    lax.fori_loop(1, devs, greet, 0)
    hid_copy = pltpu.make_async_copy(hid_hbm, hid, hid_sem)
    hid_copy.start()

    lanes = lax.broadcasted_iota(I32, (cap, 128), 1)
    for c in range(pick.shape[1] // 128):
        pick[:, c * 128:(c + 1) * 128] = jnp.where(pick_ref[...] == lanes + c * 128, 1.0, 0.0).astype(BF16)

    def make(i):
        q = turn(i)
        head_copy(q).wait()
        rows = jnp.dot(pick[...], head[q], preferred_element_type=F32).astype(BF16)
        made[2 * q] = rows[:, :cols]
        made[2 * q + 1] = rows[:, cols:]

    def give(d):
        return pltpu.make_async_remote_copy(
            src_ref=made.at[d], dst_ref=got.at[me], send_sem=made_sem.at[d], recv_sem=got_sem.at[me],
            device_id={'vocab': d}, device_id_type=pl.DeviceIdType.MESH)

    def give_chip(i):
        q = turn(i)
        give(2 * q).start()
        give(2 * q + 1).start()

    make(0)
    pl.semaphore_wait(barrier, devs - 1)

    def make_step(i, _):
        make(i)
        give_chip(i - 1)
        return 0

    lax.fori_loop(1, chips, make_step, 0)
    mate = chip * 2 + 1 - core
    part[...] = jnp.zeros_like(part)
    got[me] = made[me]
    give(mate).start()

    def got_wait(r):
        pltpu.make_async_remote_copy(
            src_ref=made.at[r], dst_ref=got.at[r], send_sem=made_sem.at[r], recv_sem=got_sem.at[r],
            device_id={'vocab': r}, device_id_type=pl.DeviceIdType.MESH).wait_recv()

    step = min(2 * cap, 256)
    band = min(256, listed)

    def place(q):
        base = q * (2 * cap)
        pair = got[pl.ds(2 * q, 2)].reshape(2 * cap, cols)
        for k in range(2 * cap // step):
            slots = pair[k * step:(k + 1) * step]
            for m in range(listed // band):
                where = code_ref[pl.ds(m * band, band), :] - base - k * step
                hot = []
                for c in range(0, step, 128):
                    w = min(128, step - c)
                    ids = lax.broadcasted_iota(I32, (band, 128), 1) + c
                    hot.append(jnp.where(where == ids, 1.0, 0.0).astype(BF16)[:, :w])
                hot = jnp.concatenate(hot, axis=1) if len(hot) > 1 else hot[0]
                part[pl.ds(m * band, band), :] += jnp.dot(hot, slots, preferred_element_type=F32)

    def place_step(i, _):
        q = lax.rem(chip + chips - 1 - i, chips)
        got_wait(2 * q)
        got_wait(2 * q + 1)
        place(q)
        return 0

    lax.fori_loop(0, chips - 1, place_step, 0)
    got_wait(mate)
    place(chip)
    gat[me] = part[...].astype(BF16)
    hid_copy.wait()
    acc[...] = jnp.zeros_like(acc)

    def piece(ref, d, h):
        return ref.at[d, pl.ds(h * half, half), :]

    def slot(a, b, h):
        return ((a % side) * side + (b % side)) * 2 + h

    sent = []

    def ring(a, b, h, da, db):
        d = dev(a % side, b % side, core)
        to = dev(da % side, db % side, core)
        copy = pltpu.make_async_remote_copy(
            src_ref=piece(gat, d, h), dst_ref=piece(gat, d, h), send_sem=ring_send.at[len(sent)],
            recv_sem=ring_recv.at[slot(a - da, b - db, h)], device_id={'vocab': to}, device_id_type=pl.DeviceIdType.MESH)
        copy.start()
        sent.append(copy)

    def pair_copy(a, b, h, c):
        d = dev(a % side, b % side, c)
        return pltpu.make_async_remote_copy(
            src_ref=piece(gat, d, h), dst_ref=piece(gat, d, h), send_sem=pair_send.at[slot(a, b, h)],
            recv_sem=pair_recv.at[slot(a, b, h)], device_id={'vocab': mate}, device_id_type=pl.DeviceIdType.MESH)

    def arrive(a, b, h):
        d = dev(a % side, b % side, core)
        pltpu.make_async_remote_copy(
            src_ref=piece(gat, d, h), dst_ref=piece(gat, d, h), send_sem=ring_send.at[0],
            recv_sem=ring_recv.at[slot(a, b, h)], device_id={'vocab': mate}, device_id_type=pl.DeviceIdType.MESH).wait_recv()

    def add(a, b):
        for h in range(2):
            pair_copy(a, b, h, 1 - core).wait_recv()
        d, e = dev(a % side, b % side, core), dev(a % side, b % side, 1 - core)

        def columns(m, _):
            at = pl.ds(pl.multiple_of(m * band, band), band)
            lhs = jnp.concatenate([hid[:, pl.ds(pl.multiple_of(d * cols, cols), cols)], hid[:, pl.ds(pl.multiple_of(e * cols, cols), cols)]], axis=1)
            rhs = jnp.concatenate([gat[d, at, :], gat[e, at, :]], axis=1)
            acc[:, at] += lax.dot_general(lhs, rhs, (((1,), (1,)), ((), ())), preferred_element_type=F32)
            return 0

        lax.fori_loop(0, listed // band, columns, 0)

    far = side // 2

    def take(a, b, h):
        if (a, b) != (0, 0):
            arrive(a, b, h)
        if b == 0:
            if a == 0:
                order = (-1, 1) if h == 0 else (1, -1)
                for s in order:
                    ring(a, b, h, s, 0)
            elif a == 1 and h == 0:
                ring(a, b, h, -1, 0)
            elif a == -1 and h == 1:
                ring(a, b, h, 1, 0)
            for s in (-1, 1):
                ring(a, b, h, 0, s)
        elif b == 1 and h == 0:
            ring(a, b, h, 0, -1)
        elif b == -1 and h == 1:
            ring(a, b, h, 0, 1)
        pair_copy(a, b, h, core).start()

    for s, h in ((-1, 0), (1, 1)):
        ring(0, 0, h, s, 0)
        ring(0, 0, h, 0, s)
    for h in range(2):
        pair_copy(0, 0, h, core).start()
    for s, h in ((-1, 1), (1, 0)):
        ring(0, 0, h, s, 0)
        ring(0, 0, h, 0, s)

    schedule = [
        ('t', 1, 0, 0), ('t', -1, 0, 1), ('t', 0, 1, 0), ('t', 0, -1, 1), ('c', 0, 0),
        ('t', 1, 0, 1), ('t', -1, 0, 0), ('t', 0, 1, 1), ('t', 0, -1, 0), ('c', 1, 0),
        ('c', -1, 0), ('c', 0, 1),
        ('t', far, 0, 0), ('t', far, 0, 1), ('c', 0, -1),
        ('t', 1, 1, 0), ('t', -1, -1, 1), ('t', -1, 1, 0), ('t', 1, -1, 1), ('c', far, 0),
        ('t', 0, far, 0), ('t', 0, far, 1),
        ('t', 1, 1, 1), ('t', -1, -1, 0), ('t', -1, 1, 1), ('t', 1, -1, 0), ('c', 0, far), ('c', 1, 1), ('c', -1, -1),
        ('t', far, 1, 0), ('t', far, -1, 1), ('c', -1, 1), ('c', 1, -1),
        ('t', far, 1, 1), ('t', far, -1, 0),
        ('t', 1, far, 0), ('t', 1, far, 1), ('c', far, 1), ('t', -1, far, 0), ('t', -1, far, 1), ('c', far, -1),
        ('c', 1, far), ('c', -1, far), ('t', far, far, 0), ('t', far, far, 1), ('c', far, far),
    ]
    for what, *at in schedule:
        if what == 't':
            take(*at)
        else:
            add(*at)

    out_copy = pltpu.make_async_copy(acc, out_hbm, out_sem)
    out_copy.start()
    for copy in sent:
        copy.wait_send()
    for a in range(side):
        for b in range(side):
            for h in range(2):
                pair_copy(a, b, h, core).wait_send()

    def given(i, _):
        give(lax.rem(me + i, devs)).wait_send()
        return 0

    lax.fori_loop(1, devs, given, 0)
    out_copy.wait()


def gather_scores(shards, cap, collective_id, hidden, w_head, allowed_ids, owner, rank):
    rows, depth = hidden.shape
    n = allowed_ids.shape[0]
    vocab_local = w_head.shape[0]
    cols = depth // shards
    side = math.isqrt(shards // 2)
    me = lax.axis_index('vocab')
    mine = (owner == me)[None, :] & (rank[None, :] == jnp.arange(cap)[:, None])
    local = jnp.sum(jnp.where(mine, (allowed_ids - me * vocab_local)[None, :] + 1, 0), axis=1) - 1
    pick = jnp.broadcast_to(local[:, None], (cap, 128))
    code = jnp.broadcast_to((owner * cap + rank)[:, None], (n, 128))
    vmem = pl.BlockSpec(memory_space=pltpu.VMEM)
    hbm = pl.BlockSpec(memory_space=pl.ANY)
    dma = pltpu.SemaphoreType.DMA
    return pl.pallas_call(
        functools.partial(gather_kernel, side, cap),
        out_shape=jax.ShapeDtypeStruct((rows, n), F32),
        in_specs=[hbm, hbm, vmem, vmem],
        out_specs=hbm,
        scratch_shapes=[
            pltpu.VMEM((rows, depth), BF16),
            pltpu.VMEM((shards // 2, vocab_local, 2 * cols), BF16),
            pltpu.VMEM((cap, vocab_local), BF16),
            pltpu.VMEM((shards, cap, cols), BF16),
            pltpu.VMEM((shards, cap, cols), BF16),
            pltpu.VMEM((n, cols), F32),
            pltpu.VMEM((shards, n, cols), BF16),
            pltpu.VMEM((rows, n), F32),
            dma, dma((shards // 2,)), dma((shards,)), dma((shards,)),
            dma((30,)), dma((shards,)), dma((shards,)), dma((shards,)), dma,
        ],
        compiler_params=pltpu.CompilerParams(collective_id=collective_id, has_side_effects=True, vmem_limit_bytes=60 * 1024 * 1024),
        name=f'gather_scores_{cap}',
    )(hidden, w_head, pick, code)


def solution(mesh):
    shards = mesh.shape['vocab']

    def device_step(hidden, w_head, allowed_ids, allowed_valid, target_pos):
        vocab_local = w_head.shape[0]
        n = allowed_ids.shape[0]
        owner = allowed_ids // vocab_local
        rank, counts = ranks(owner, shards)
        caps = (2 * n // shards, vocab_local)
        run = [functools.partial(gather_scores, shards, cap, i) for i, cap in enumerate(caps)]
        scores = lax.cond(jnp.max(counts) <= caps[0], *run, hidden, w_head, allowed_ids, owner, rank) * INV_TEMP
        keep = (allowed_valid > 0)[None, :]
        masked = jnp.where(keep, scores, -jnp.inf)
        log_norm = jax.nn.logsumexp(masked, axis=1)
        probs = jnp.where(keep, jnp.exp(masked - log_norm[:, None]), 0.0)
        hit = target_pos[:, None] == jnp.arange(n)[None, :]
        picked = jnp.sum(jnp.where(hit, scores, 0.0), axis=1)
        return probs, picked - log_norm

    row_spec = P(('rep', 'vocab'))
    mat_spec = P(('rep', 'vocab'), None)
    return jax.shard_map(device_step, mesh=mesh, in_specs=(mat_spec, P('vocab', None), P('rep'), P('rep'), row_spec), out_specs=(mat_spec, row_spec), check_vma=False)
```

```python
import functools
import math

import jax
import jax.numpy as jnp
from jax import lax
from jax.experimental import pallas as pl
from jax.experimental.pallas import tpu as pltpu
from jax.sharding import PartitionSpec as P

INV_TEMP = 1.25
LEAD = 2
F32, BF16, I32 = jnp.float32, jnp.bfloat16, jnp.int32


def column(row):
    return jnp.transpose(jnp.broadcast_to(row, (128, 128)))


def lane_ids(rows):
    return lax.broadcasted_iota(I32, (rows, 128), 1)


def prepare(me, shards, vocab_local, cap, ids_ref, code_ref, pick):
    lanes = lane_ids(128)
    below = (lax.broadcasted_iota(I32, (128, 128), 0) > lanes).astype(F32).astype(BF16)
    before = jnp.zeros((1, 128), F32)
    mine = [jnp.zeros((1, 128), F32) for _ in range(-(-cap // 128))]
    for b in range(ids_ref.shape[0]):
        ids = column(ids_ref[b:b + 1, :].astype(F32)).astype(I32)
        owner = ids >> (vocab_local.bit_length() - 1) if vocab_local & (vocab_local - 1) == 0 else ids // vocab_local
        hot = (owner == lanes).astype(F32)
        number = jnp.dot(below, hot.astype(BF16), preferred_element_type=F32) + before
        before = before + jnp.sum(hot, axis=0, keepdims=True)
        number = jnp.sum(hot * number, axis=1, keepdims=True).astype(I32)
        code = owner * cap + number
        code_ref[b * 128:(b + 1) * 128, :] = code
        local = (ids - me * vocab_local + 1).astype(F32)
        for c in range(len(mine)):
            mine[c] += jnp.sum(jnp.where(code == lanes + (me * cap + c * 128), local, 0.0), axis=0, keepdims=True)
    for c in range(len(mine)):
        rows = min(128, cap - c * 128)
        local = (column(mine[c]) - 1.0).astype(I32)[:rows]
        for k in range(0, vocab_local, 128):
            pick[c * 128:c * 128 + rows, k:k + 128] = (local == lane_ids(rows) + k).astype(F32).astype(BF16)


def gather_kernel(side, cap, lead, group, hid_hbm, head_hbm, ids_ref, out_hbm,
                  hid, head, code_ref, pick, made, got, part, gat, acc,
                  hid_sem, head_sem, made_sem, got_sem, ring_send, ring_recv, pair_send, pair_recv, out_sem):
    chips = side * side
    devs = 2 * chips
    cols = made.shape[2]
    listed = gat.shape[1]
    half = listed // 2
    me = lax.axis_index('vocab')
    core = lax.rem(me, 2)
    chip = me // 2
    x, y = lax.rem(chip, side), chip // side

    def dev(a, b, c):
        px = lax.rem(x + a * (1 - c) + b * c, side)
        py = lax.rem(y + a * c + b * (1 - c), side)
        return (py * side + px) * 2 + c

    barrier = pltpu.get_barrier_semaphore()

    def greet(i, _):
        pl.semaphore_signal(barrier, inc=1, device_id={'vocab': lax.rem(me + i, devs)}, device_id_type=pl.DeviceIdType.MESH)
        return 0

    def turn(i):
        return lax.rem(chip + 1 + i, chips)

    def head_copy(q):
        return pltpu.make_async_copy(head_hbm.at[:, pl.ds(pl.multiple_of(q * 2 * cols, 2 * cols), 2 * cols)], head.at[q], head_sem.at[q])

    def head_start(i, _):
        head_copy(turn(i)).start()
        return 0

    lax.fori_loop(1, devs, greet, 0)
    lax.fori_loop(0, chips, head_start, 0)
    hid_copy = pltpu.make_async_copy(hid_hbm, hid, hid_sem)
    hid_copy.start()

    prepare(me, devs, head.shape[1], cap, ids_ref, code_ref, pick)

    def make(i):
        q = turn(i)
        head_copy(q).wait()
        rows = jnp.dot(pick[...], head[q], preferred_element_type=F32).astype(BF16)
        made[2 * q] = rows[:, :cols]
        made[2 * q + 1] = rows[:, cols:]

    def give(d):
        return pltpu.make_async_remote_copy(
            src_ref=made.at[d], dst_ref=got.at[me], send_sem=made_sem.at[d], recv_sem=got_sem.at[me],
            device_id={'vocab': d}, device_id_type=pl.DeviceIdType.MESH)

    def give_chip(i):
        q = turn(i)
        give(2 * q).start()
        give(2 * q + 1).start()

    def make_only(i, _):
        make(i)
        return 0

    def make_give(i, _):
        make(i)
        give_chip(i - lead)
        return 0

    def give_only(i, _):
        give_chip(i)
        return 0

    lax.fori_loop(0, lead, make_only, 0)
    pl.semaphore_wait(barrier, devs - 1)
    lax.fori_loop(lead, chips, make_give, 0)
    lax.fori_loop(chips - lead, chips - 1, give_only, 0)
    mate = chip * 2 + 1 - core
    part[...] = jnp.zeros_like(part)
    got[me] = made[me]
    give(mate).start()

    def got_wait(r):
        pltpu.make_async_remote_copy(
            src_ref=made.at[r], dst_ref=got.at[r], send_sem=made_sem.at[r], recv_sem=got_sem.at[r],
            device_id={'vocab': r}, device_id_type=pl.DeviceIdType.MESH).wait_recv()

    step = min(2 * cap, 256)
    band = min(256, listed)
    wide = listed if group > 1 else band

    def place(q):
        base = q * (2 * cap)
        pair = got[pl.ds(2 * q, 2)].reshape(2 * cap, cols)
        for k in range(2 * cap // step):
            slots = pair[k * step:(k + 1) * step]
            for m in range(listed // band):
                where = code_ref[pl.ds(m * band, band), :] - base - k * step
                hot = []
                for c in range(0, step, 128):
                    w = min(128, step - c)
                    ids = lax.broadcasted_iota(I32, (band, 128), 1) + c
                    hot.append(jnp.where(where == ids, 1.0, 0.0).astype(BF16)[:, :w])
                hot = jnp.concatenate(hot, axis=1) if len(hot) > 1 else hot[0]
                part[pl.ds(m * band, band), :] += jnp.dot(hot, slots, preferred_element_type=F32)

    def place_step(i, _):
        q = lax.rem(chip + chips - 1 - i, chips)
        got_wait(2 * q)
        got_wait(2 * q + 1)
        place(q)
        return 0

    lax.fori_loop(0, chips - 1, place_step, 0)
    got_wait(mate)
    place(chip)
    gat[me] = part[...].astype(BF16)
    hid_copy.wait()
    acc[...] = jnp.zeros_like(acc)

    def piece(ref, d, h):
        return ref.at[d, pl.ds(h * half, half), :]

    def slot(a, b, h):
        return ((a % side) * side + (b % side)) * 2 + h

    sent = []

    def ring_copy(k, a, b, h, da, db):
        d = dev(a % side, b % side, core)
        to = dev(da % side, db % side, core)
        return pltpu.make_async_remote_copy(
            src_ref=piece(gat, d, h), dst_ref=piece(gat, d, h), send_sem=ring_send.at[k],
            recv_sem=ring_recv.at[slot(a - da, b - db, h)], device_id={'vocab': to}, device_id_type=pl.DeviceIdType.MESH)

    def ring(*at):
        ring_copy(len(sent), *at).start()
        sent.append(at)

    def pair_copy(a, b, h, c):
        d = dev(a % side, b % side, c)
        return pltpu.make_async_remote_copy(
            src_ref=piece(gat, d, h), dst_ref=piece(gat, d, h), send_sem=pair_send.at[slot(a, b, h)],
            recv_sem=pair_recv.at[slot(a, b, h)], device_id={'vocab': mate}, device_id_type=pl.DeviceIdType.MESH)

    def arrive(a, b, h):
        d = dev(a % side, b % side, core)
        pltpu.make_async_remote_copy(
            src_ref=piece(gat, d, h), dst_ref=piece(gat, d, h), send_sem=ring_send.at[0],
            recv_sem=ring_recv.at[slot(a, b, h)], device_id={'vocab': mate}, device_id_type=pl.DeviceIdType.MESH).wait_recv()

    def ready(a, b):
        for h in range(2):
            pair_copy(a, b, h, 1 - core).wait_recv()

    def add(slices):
        lhs = jnp.concatenate([hid[:, pl.ds(pl.multiple_of(d * cols, cols), cols)] for d in slices], axis=1)
        for m in range(0, listed, wide):
            rhs = jnp.concatenate([gat[d, m:m + wide, :] for d in slices], axis=1)
            acc[:, m:m + wide] += lax.dot_general(lhs, rhs, (((1,), (1,)), ((), ())), preferred_element_type=F32)

    far = side // 2

    def take(a, b, h):
        if (a, b) != (0, 0):
            arrive(a, b, h)
        if b == 0:
            if a == 0:
                order = (-1, 1) if h == 0 else (1, -1)
                for s in order:
                    ring(a, b, h, s, 0)
            elif a == 1 and h == 0:
                ring(a, b, h, -1, 0)
            elif a == -1 and h == 1:
                ring(a, b, h, 1, 0)
            for s in (-1, 1):
                ring(a, b, h, 0, s)
        elif b == 1 and h == 0:
            ring(a, b, h, 0, -1)
        elif b == -1 and h == 1:
            ring(a, b, h, 0, 1)
        pair_copy(a, b, h, core).start()

    for s, h in ((-1, 0), (1, 1)):
        ring(0, 0, h, s, 0)
        ring(0, 0, h, 0, s)
    for h in range(2):
        pair_copy(0, 0, h, core).start()
    for s, h in ((-1, 1), (1, 0)):
        ring(0, 0, h, s, 0)
        ring(0, 0, h, 0, s)

    phases = [
        ([(1, 0, 0), (-1, 0, 1), (0, 1, 0), (0, -1, 1), (1, 0, 1), (-1, 0, 0), (0, 1, 1), (0, -1, 0)], [(0, 0), (1, 0)]),
        ([], [(-1, 0), (0, 1)]),
        ([(far, 0, 0), (far, 0, 1)], [(0, -1), (far, 0)]),
        ([(1, 1, 0), (-1, -1, 1), (-1, 1, 0), (1, -1, 1), (0, far, 0), (0, far, 1), (1, 1, 1), (-1, -1, 0)], [(0, far), (1, 1)]),
        ([(-1, 1, 1), (1, -1, 0), (far, 1, 0), (far, -1, 1)], [(-1, -1), (-1, 1)]),
        ([(far, 1, 1), (far, -1, 0), (1, far, 0), (1, far, 1)], [(1, -1), (far, 1)]),
        ([(-1, far, 0), (-1, far, 1)], [(far, -1), (1, far)]),
        ([(far, far, 0), (far, far, 1)], [(-1, far), (far, far)]),
    ]

    def phase(p, _):
        at = [0] * 4
        for k, (takes, adds) in enumerate(phases):
            @pl.when(p == k)
            def _():
                for t in takes:
                    take(*t)
                for t in adds:
                    ready(*t)
            for i, v in enumerate(sum(adds, ())):
                at[i] = at[i] + (p == k).astype(I32) * (v % side)
        slices = [dev(at[0], at[1], core), dev(at[0], at[1], 1 - core), dev(at[2], at[3], core), dev(at[2], at[3], 1 - core)]
        for g in range(0, 4, 2 * group):
            add(slices[g:g + 2 * group])
        return 0

    lax.fori_loop(0, len(phases), phase, 0)

    out_copy = pltpu.make_async_copy(acc, out_hbm, out_sem)
    out_copy.start()
    for k, at in enumerate(sent):
        ring_copy(k, *at).wait_send()
    for a in range(side):
        for b in range(side):
            for h in range(2):
                pair_copy(a, b, h, core).wait_send()

    def given(i, _):
        give(lax.rem(me + i, devs)).wait_send()
        return 0

    lax.fori_loop(1, devs, given, 0)
    out_copy.wait()


def gather_scores(shards, cap, group, collective_id, hidden, w_head, ids):
    rows, depth = hidden.shape
    n = ids.shape[0] * ids.shape[1]
    vocab_local = w_head.shape[0]
    cols = depth // shards
    side = math.isqrt(shards // 2)
    vmem = pl.BlockSpec(memory_space=pltpu.VMEM)
    hbm = pl.BlockSpec(memory_space=pl.ANY)
    dma = pltpu.SemaphoreType.DMA
    return pl.pallas_call(
        functools.partial(gather_kernel, side, cap, LEAD, group),
        out_shape=jax.ShapeDtypeStruct((rows, n), F32),
        in_specs=[hbm, hbm, vmem],
        out_specs=hbm,
        scratch_shapes=[
            pltpu.VMEM((rows, depth), BF16),
            pltpu.VMEM((shards // 2, vocab_local, 2 * cols), BF16),
            pltpu.VMEM((n, 128), I32),
            pltpu.VMEM((cap, vocab_local), BF16),
            pltpu.VMEM((shards, cap, cols), BF16),
            pltpu.VMEM((shards, cap, cols), BF16),
            pltpu.VMEM((n, cols), F32),
            pltpu.VMEM((shards, n, cols), BF16),
            pltpu.VMEM((rows, n), F32),
            dma, dma((shards // 2,)), dma((shards,)), dma((shards,)),
            dma((30,)), dma((shards,)), dma((shards,)), dma((shards,)), dma,
        ],
        compiler_params=pltpu.CompilerParams(collective_id=collective_id, has_side_effects=True, vmem_limit_bytes=60 * 1024 * 1024),
        name=f'gather_scores_{cap}',
    )(hidden, w_head, ids)


def finish_kernel(score_ref, valid_ref, target_ref, probs_ref, logp_ref):
    rows, n = score_ref.shape
    keep = valid_ref[...] > 0
    scores = score_ref[...] * INV_TEMP
    top = jnp.max(jnp.where(keep, scores, -jnp.inf), axis=1, keepdims=True)
    terms = jnp.where(keep, jnp.exp(scores - top), 0.0)
    total = jnp.sum(terms, axis=1, keepdims=True)
    probs_ref[...] = terms * (1.0 / total)
    target = column(target_ref[0].astype(F32)).astype(I32)[:rows]
    picked = jnp.zeros((rows, 128), F32)
    for c in range(0, n, 128):
        picked += jnp.where(target == lane_ids(rows) + c, scores[:, c:c + 128], 0.0)
    logp = jnp.sum(picked, axis=1, keepdims=True) - (top + jnp.log(total))
    logp_ref[0] = jnp.transpose(jnp.broadcast_to(logp, (rows, 128)))[:1]


def finish(scores, allowed_valid, target_pos):
    rows, n = scores.shape
    block = min(128, rows)
    probs, logp = pl.pallas_call(
        finish_kernel,
        grid=(rows // block,),
        out_shape=(jax.ShapeDtypeStruct((rows, n), F32), jax.ShapeDtypeStruct((rows // block, 1, block), F32)),
        in_specs=[pl.BlockSpec((block, n), lambda i: (i, 0)), pl.BlockSpec((1, n), lambda i: (0, 0)),
                  pl.BlockSpec((1, 1, block), lambda i: (i, 0, 0))],
        out_specs=(pl.BlockSpec((block, n), lambda i: (i, 0)), pl.BlockSpec((1, 1, block), lambda i: (i, 0, 0))),
        compiler_params=pltpu.CompilerParams(dimension_semantics=('arbitrary',)),
        name='finish',
    )(scores, allowed_valid.reshape(1, n), target_pos.reshape(rows // block, 1, block))
    return probs, logp.reshape(rows)


def solution(mesh):
    shards = mesh.shape['vocab']

    def device_step(hidden, w_head, allowed_ids, allowed_valid, target_pos):
        vocab_local = w_head.shape[0]
        n = allowed_ids.shape[0]
        counts = jnp.sum((allowed_ids // vocab_local)[None, :] == jnp.arange(shards)[:, None], axis=1)
        caps = (2 * n // shards, vocab_local)
        run = [functools.partial(gather_scores, shards, cap, 2 - i, i) for i, cap in enumerate(caps)]
        scores = lax.cond(jnp.max(counts) <= caps[0], *run, hidden, w_head, allowed_ids.reshape(n // 128, 128))
        return finish(scores, allowed_valid, target_pos)

    row_spec = P(('rep', 'vocab'))
    mat_spec = P(('rep', 'vocab'), None)
    return jax.shard_map(device_step, mesh=mesh, in_specs=(mat_spec, P('vocab', None), P('rep'), P('rep'), row_spec), out_specs=(mat_spec, row_spec), check_vma=False)
```

```python
import functools
import math

import jax
import jax.numpy as jnp
from jax import lax
from jax.experimental import pallas as pl
from jax.experimental.pallas import tpu as pltpu
from jax.sharding import PartitionSpec as P

INV_TEMP = 1.25
LEAD = 2
F32, BF16, I32 = jnp.float32, jnp.bfloat16, jnp.int32


def column(row):
    return jnp.transpose(jnp.broadcast_to(row, (128, 128)))


def lane_ids(rows):
    return lax.broadcasted_iota(I32, (rows, 128), 1)


def prepare(me, shards, vocab_local, cap, ids_ref, code_ref, pick):
    lanes = lane_ids(128)
    below = (lax.broadcasted_iota(I32, (128, 128), 0) > lanes).astype(F32).astype(BF16)
    before = jnp.zeros((1, 128), F32)
    mine = [jnp.zeros((1, 128), F32) for _ in range(-(-cap // 128))]
    for b in range(ids_ref.shape[0]):
        ids = column(ids_ref[b:b + 1, :].astype(F32)).astype(I32)
        owner = ids >> (vocab_local.bit_length() - 1) if vocab_local & (vocab_local - 1) == 0 else ids // vocab_local
        hot = (owner == lanes).astype(F32)
        number = jnp.dot(below, hot.astype(BF16), preferred_element_type=F32) + before
        before = before + jnp.sum(hot, axis=0, keepdims=True)
        number = jnp.sum(hot * number, axis=1, keepdims=True).astype(I32)
        code = owner * cap + number
        code_ref[b * 128:(b + 1) * 128, :] = code
        local = (ids - me * vocab_local + 1).astype(F32)
        for c in range(len(mine)):
            mine[c] += jnp.sum(jnp.where(code == lanes + (me * cap + c * 128), local, 0.0), axis=0, keepdims=True)
    for c in range(len(mine)):
        rows = min(128, cap - c * 128)
        local = (column(mine[c]) - 1.0).astype(I32)[:rows]
        for k in range(0, vocab_local, 128):
            pick[c * 128:c * 128 + rows, k:k + 128] = (local == lane_ids(rows) + k).astype(F32).astype(BF16)


def gather_kernel(side, cap, lead, group, hid_hbm, head_hbm, ids_ref, acc,
                  hid, head, code_ref, pick, made, got, part, gat,
                  hid_sem, head_sem, made_sem, got_sem, ring_send, ring_recv, pair_send, pair_recv):
    chips = side * side
    devs = 2 * chips
    cols = made.shape[2]
    listed = gat.shape[1]
    half = listed // 2
    me = lax.axis_index('vocab')
    core = lax.rem(me, 2)
    chip = me // 2
    x, y = lax.rem(chip, side), chip // side

    def dev(a, b, c):
        px = lax.rem(x + a * (1 - c) + b * c, side)
        py = lax.rem(y + a * c + b * (1 - c), side)
        return (py * side + px) * 2 + c

    barrier = pltpu.get_barrier_semaphore()

    def greet(i, _):
        pl.semaphore_signal(barrier, inc=1, device_id={'vocab': lax.rem(me + i, devs)}, device_id_type=pl.DeviceIdType.MESH)
        return 0

    def turn(i):
        return lax.rem(chip + 1 + i, chips)

    def head_copy(q):
        return pltpu.make_async_copy(head_hbm.at[:, pl.ds(pl.multiple_of(q * 2 * cols, 2 * cols), 2 * cols)], head.at[q], head_sem.at[q])

    def head_start(i, _):
        head_copy(turn(i)).start()
        return 0

    lax.fori_loop(1, devs, greet, 0)
    lax.fori_loop(0, chips, head_start, 0)
    hid_copy = pltpu.make_async_copy(hid_hbm, hid, hid_sem)
    hid_copy.start()

    prepare(me, devs, head.shape[1], cap, ids_ref, code_ref, pick)

    def make(i):
        q = turn(i)
        head_copy(q).wait()
        rows = jnp.dot(pick[...], head[q], preferred_element_type=F32).astype(BF16)
        made[2 * q] = rows[:, :cols]
        made[2 * q + 1] = rows[:, cols:]

    def give(d):
        return pltpu.make_async_remote_copy(
            src_ref=made.at[d], dst_ref=got.at[me], send_sem=made_sem.at[d], recv_sem=got_sem.at[me],
            device_id={'vocab': d}, device_id_type=pl.DeviceIdType.MESH)

    def give_chip(i):
        q = turn(i)
        give(2 * q).start()
        give(2 * q + 1).start()

    def make_only(i, _):
        make(i)
        return 0

    def make_give(i, _):
        make(i)
        give_chip(i - lead)
        return 0

    def give_only(i, _):
        give_chip(i)
        return 0

    lax.fori_loop(0, lead, make_only, 0)
    pl.semaphore_wait(barrier, devs - 1)
    lax.fori_loop(lead, chips, make_give, 0)
    lax.fori_loop(chips - lead, chips - 1, give_only, 0)
    mate = chip * 2 + 1 - core
    part[...] = jnp.zeros_like(part)
    got[me] = made[me]
    give(mate).start()

    def got_wait(r):
        pltpu.make_async_remote_copy(
            src_ref=made.at[r], dst_ref=got.at[r], send_sem=made_sem.at[r], recv_sem=got_sem.at[r],
            device_id={'vocab': r}, device_id_type=pl.DeviceIdType.MESH).wait_recv()

    step = min(2 * cap, 256)
    band = min(256, listed)
    wide = listed if group > 1 else band

    def place(q):
        base = q * (2 * cap)
        pair = got[pl.ds(2 * q, 2)].reshape(2 * cap, cols)
        for k in range(2 * cap // step):
            slots = pair[k * step:(k + 1) * step]
            for m in range(listed // band):
                where = code_ref[pl.ds(m * band, band), :] - base - k * step
                hot = []
                for c in range(0, step, 128):
                    w = min(128, step - c)
                    ids = lax.broadcasted_iota(I32, (band, 128), 1) + c
                    hot.append(jnp.where(where == ids, 1.0, 0.0).astype(BF16)[:, :w])
                hot = jnp.concatenate(hot, axis=1) if len(hot) > 1 else hot[0]
                part[pl.ds(m * band, band), :] += jnp.dot(hot, slots, preferred_element_type=F32)

    def place_step(i, _):
        q = lax.rem(chip + chips - 1 - i, chips)
        got_wait(2 * q)
        got_wait(2 * q + 1)
        place(q)
        return 0

    lax.fori_loop(0, chips - 1, place_step, 0)
    got_wait(mate)
    place(chip)
    gat[me] = part[...].astype(BF16)
    hid_copy.wait()
    acc[...] = jnp.zeros_like(acc)

    def piece(ref, d, h):
        return ref.at[d, pl.ds(h * half, half), :]

    def slot(a, b, h):
        return ((a % side) * side + (b % side)) * 2 + h

    sent = []

    def ring_copy(k, a, b, h, da, db):
        d = dev(a % side, b % side, core)
        to = dev(da % side, db % side, core)
        return pltpu.make_async_remote_copy(
            src_ref=piece(gat, d, h), dst_ref=piece(gat, d, h), send_sem=ring_send.at[k],
            recv_sem=ring_recv.at[slot(a - da, b - db, h)], device_id={'vocab': to}, device_id_type=pl.DeviceIdType.MESH)

    def ring(*at):
        ring_copy(len(sent), *at).start()
        sent.append(at)

    def pair_copy(a, b, h, c):
        d = dev(a % side, b % side, c)
        return pltpu.make_async_remote_copy(
            src_ref=piece(gat, d, h), dst_ref=piece(gat, d, h), send_sem=pair_send.at[slot(a, b, h)],
            recv_sem=pair_recv.at[slot(a, b, h)], device_id={'vocab': mate}, device_id_type=pl.DeviceIdType.MESH)

    def arrive(a, b, h):
        d = dev(a % side, b % side, core)
        pltpu.make_async_remote_copy(
            src_ref=piece(gat, d, h), dst_ref=piece(gat, d, h), send_sem=ring_send.at[0],
            recv_sem=ring_recv.at[slot(a, b, h)], device_id={'vocab': mate}, device_id_type=pl.DeviceIdType.MESH).wait_recv()

    def ready(a, b):
        for h in range(2):
            pair_copy(a, b, h, 1 - core).wait_recv()

    def add(slices):
        lhs = jnp.concatenate([hid[:, pl.ds(pl.multiple_of(d * cols, cols), cols)] for d in slices], axis=1)
        for m in range(0, listed, wide):
            rhs = jnp.concatenate([gat[d, m:m + wide, :] for d in slices], axis=1)
            acc[:, m:m + wide] += lax.dot_general(lhs, rhs, (((1,), (1,)), ((), ())), preferred_element_type=F32)

    far = side // 2

    def take(a, b, h):
        if (a, b) != (0, 0):
            arrive(a, b, h)
        if b == 0:
            if a == 0:
                order = (-1, 1) if h == 0 else (1, -1)
                for s in order:
                    ring(a, b, h, s, 0)
            elif a == 1 and h == 0:
                ring(a, b, h, -1, 0)
            elif a == -1 and h == 1:
                ring(a, b, h, 1, 0)
            for s in (-1, 1):
                ring(a, b, h, 0, s)
        elif b == 1 and h == 0:
            ring(a, b, h, 0, -1)
        elif b == -1 and h == 1:
            ring(a, b, h, 0, 1)
        pair_copy(a, b, h, core).start()

    for s, h in ((-1, 0), (1, 1)):
        ring(0, 0, h, s, 0)
        ring(0, 0, h, 0, s)
    for h in range(2):
        pair_copy(0, 0, h, core).start()
    for s, h in ((-1, 1), (1, 0)):
        ring(0, 0, h, s, 0)
        ring(0, 0, h, 0, s)

    phases = [
        ([(1, 0, 0), (-1, 0, 1), (0, 1, 0), (0, -1, 1), (1, 0, 1), (-1, 0, 0), (0, 1, 1), (0, -1, 0)], [(0, 0), (1, 0)]),
        ([], [(-1, 0), (0, 1)]),
        ([(far, 0, 0), (far, 0, 1)], [(0, -1), (far, 0)]),
        ([(1, 1, 0), (-1, -1, 1), (-1, 1, 0), (1, -1, 1), (0, far, 0), (0, far, 1), (1, 1, 1), (-1, -1, 0)], [(0, far), (1, 1)]),
        ([(-1, 1, 1), (1, -1, 0), (far, 1, 0), (far, -1, 1)], [(-1, -1), (-1, 1)]),
        ([(far, 1, 1), (far, -1, 0), (1, far, 0), (1, far, 1)], [(1, -1), (far, 1)]),
        ([(-1, far, 0), (-1, far, 1)], [(far, -1), (1, far)]),
        ([(far, far, 0), (far, far, 1)], [(-1, far), (far, far)]),
    ]

    def phase(p, _):
        at = [0] * 4
        for k, (takes, adds) in enumerate(phases):
            @pl.when(p == k)
            def _():
                for t in takes:
                    take(*t)
                for t in adds:
                    ready(*t)
            for i, v in enumerate(sum(adds, ())):
                at[i] = at[i] + (p == k).astype(I32) * (v % side)
        slices = [dev(at[0], at[1], core), dev(at[0], at[1], 1 - core), dev(at[2], at[3], core), dev(at[2], at[3], 1 - core)]
        for g in range(0, 4, 2 * group):
            add(slices[g:g + 2 * group])
        return 0

    lax.fori_loop(0, len(phases), phase, 0)

    for k, at in enumerate(sent):
        ring_copy(k, *at).wait_send()
    for a in range(side):
        for b in range(side):
            for h in range(2):
                pair_copy(a, b, h, core).wait_send()

    def given(i, _):
        give(lax.rem(me + i, devs)).wait_send()
        return 0

    lax.fori_loop(1, devs, given, 0)


def gather_scores(shards, cap, group, collective_id, hidden, w_head, ids):
    rows, depth = hidden.shape
    n = ids.shape[0] * ids.shape[1]
    vocab_local = w_head.shape[0]
    cols = depth // shards
    side = math.isqrt(shards // 2)
    vmem = pl.BlockSpec(memory_space=pltpu.VMEM)
    hbm = pl.BlockSpec(memory_space=pl.ANY)
    dma = pltpu.SemaphoreType.DMA
    limit = 2 * (rows * depth + vocab_local * depth + cap * (vocab_local + 2 * depth) + n * depth + 4 * n * cols) + 8 * 1024 * 1024
    return pl.pallas_call(
        functools.partial(gather_kernel, side, cap, LEAD, group),
        out_shape=jax.ShapeDtypeStruct((rows, n), F32),
        in_specs=[hbm, hbm, vmem],
        out_specs=vmem,
        scratch_shapes=[
            pltpu.VMEM((rows, depth), BF16),
            pltpu.VMEM((shards // 2, vocab_local, 2 * cols), BF16),
            pltpu.VMEM((n, 128), I32),
            pltpu.VMEM((cap, vocab_local), BF16),
            pltpu.VMEM((shards, cap, cols), BF16),
            pltpu.VMEM((shards, cap, cols), BF16),
            pltpu.VMEM((n, cols), F32),
            pltpu.VMEM((shards, n, cols), BF16),
            dma, dma((shards // 2,)), dma((shards,)), dma((shards,)),
            dma((30,)), dma((shards,)), dma((shards,)), dma((shards,)),
        ],
        compiler_params=pltpu.CompilerParams(collective_id=collective_id, has_side_effects=True, vmem_limit_bytes=limit),
        name=f'gather_scores_{cap}',
    )(hidden, w_head, ids)


def finish_kernel(score_ref, valid_ref, target_ref, probs_ref, logp_ref):
    rows, n = probs_ref.shape
    keep = valid_ref[...] > 0
    scores = score_ref[pl.ds(pl.multiple_of(pl.program_id(0) * rows, rows), rows), :] * INV_TEMP
    top = jnp.max(jnp.where(keep, scores, -jnp.inf), axis=1, keepdims=True)
    terms = jnp.where(keep, jnp.exp(scores - top), 0.0)
    total = jnp.sum(terms, axis=1, keepdims=True)
    probs_ref[...] = terms * (1.0 / total)
    target = column(target_ref[0].astype(F32)).astype(I32)[:rows]
    picked = jnp.zeros((rows, 128), F32)
    for c in range(0, n, 128):
        picked += jnp.where(target == lane_ids(rows) + c, scores[:, c:c + 128], 0.0)
    logp = jnp.sum(picked, axis=1, keepdims=True) - (top + jnp.log(total))
    logp_ref[0] = jnp.transpose(jnp.broadcast_to(logp, (rows, 128)))[:1]


def finish(scores, allowed_valid, target_pos):
    rows, n = scores.shape
    block = min(128, rows)
    probs, logp = pl.pallas_call(
        finish_kernel,
        grid=(rows // block,),
        out_shape=(jax.ShapeDtypeStruct((rows, n), F32), jax.ShapeDtypeStruct((rows // block, 1, block), F32)),
        in_specs=[pl.BlockSpec(memory_space=pltpu.VMEM), pl.BlockSpec((1, n), lambda i: (0, 0)),
                  pl.BlockSpec((1, 1, block), lambda i: (i, 0, 0))],
        out_specs=(pl.BlockSpec((block, n), lambda i: (i, 0)), pl.BlockSpec((1, 1, block), lambda i: (i, 0, 0))),
        compiler_params=pltpu.CompilerParams(dimension_semantics=('arbitrary',), vmem_limit_bytes=16 * 1024 * 1024),
        name='finish',
    )(scores, allowed_valid.reshape(1, n), target_pos.reshape(rows // block, 1, block))
    return probs, logp.reshape(rows)


def solution(mesh):
    shards = mesh.shape['vocab']

    def device_step(hidden, w_head, allowed_ids, allowed_valid, target_pos):
        vocab_local = w_head.shape[0]
        n = allowed_ids.shape[0]
        counts = jnp.sum((allowed_ids // vocab_local)[None, :] == jnp.arange(shards)[:, None], axis=1)
        caps = (2 * n // shards, vocab_local)

        def run(i, cap):
            return lambda hidden, w_head, ids, valid, target: finish(gather_scores(shards, cap, 2 - i, i, hidden, w_head, ids), valid, target)

        runs = [run(i, cap) for i, cap in enumerate(caps)]
        return lax.cond(jnp.max(counts) <= caps[0], *runs, hidden, w_head, allowed_ids.reshape(n // 128, 128), allowed_valid, target_pos)

    row_spec = P(('rep', 'vocab'))
    mat_spec = P(('rep', 'vocab'), None)
    return jax.shard_map(device_step, mesh=mesh, in_specs=(mat_spec, P('vocab', None), P('rep'), P('rep'), row_spec), out_specs=(mat_spec, row_spec), check_vma=False)
```

```python
import functools
import math

import jax
import jax.numpy as jnp
from jax import lax
from jax.experimental import pallas as pl
from jax.experimental.pallas import tpu as pltpu
from jax.sharding import PartitionSpec as P

INV_TEMP = 1.25
SIZES = (5, 6, 7, 8)
LEAD = 2
F32, BF16, I32 = jnp.float32, jnp.bfloat16, jnp.int32


def column(row):
    return jnp.transpose(jnp.broadcast_to(row, (128, 128)))


def lane_ids(rows):
    return lax.broadcasted_iota(I32, (rows, 128), 1)


def power_div(value, by):
    return value >> (by.bit_length() - 1) if by & (by - 1) == 0 else value // by


def prepare(me, vocab_local, cap, ids_ref, valid_ref, code_ref, pos_ref, pick):
    lanes = lane_ids(128)
    below = (lax.broadcasted_iota(I32, (128, 128), 0) > lanes).astype(F32).astype(BF16)
    before = jnp.zeros((1, 128), F32)
    mine = [jnp.zeros((1, 128), F32) for _ in range(-(-cap // 128))]
    for b in range(ids_ref.shape[0]):
        ids = jnp.where(valid_ref[b:b + 1, :] > 0, ids_ref[b:b + 1, :], -1)
        ids = column(ids.astype(F32)).astype(I32)
        valid = ids >= 0
        owner = jnp.where(valid, power_div(ids, vocab_local), -1)
        own = (owner == lanes).astype(F32)
        hot = jnp.where((lanes == 127) & valid, 1.0, own)
        number = jnp.dot(below, hot.astype(BF16), preferred_element_type=F32) + before
        before = before + jnp.sum(hot, axis=0, keepdims=True)
        pos = jnp.sum(jnp.where(lanes == 127, number, 0.0), axis=1, keepdims=True).astype(I32)
        number = jnp.sum(own * number, axis=1, keepdims=True).astype(I32)
        code = jnp.where(valid, owner * cap + number, -1)
        code_ref[b * 128:(b + 1) * 128, :] = code
        pos_ref[b * 128:(b + 1) * 128, :] = jnp.where(valid, pos, -1)
        local = (ids - me * vocab_local + 1).astype(F32)
        for c in range(len(mine)):
            mine[c] += jnp.sum(jnp.where(code == lanes + (me * cap + c * 128), local, 0.0), axis=0, keepdims=True)
    for c in range(len(mine)):
        rows = min(128, cap - c * 128)
        local = (column(mine[c]) - 1.0).astype(I32)[:rows]
        for k in range(0, vocab_local, 128):
            pick[c * 128:c * 128 + rows, k:k + 128] = (local == lane_ids(rows) + k).astype(F32).astype(BF16)


def compact(code_ref, pos_ref, slot_ref):
    def block(b, total, k):
        at = pl.ds(pl.multiple_of(b * 128, 128), 128)
        here = jnp.where(pos_ref[at, :] == lane_ids(128) + k * 128, code_ref[at, :] + 1, 0)
        return total + jnp.sum(here.reshape(16, 8, 128), axis=0)

    for k in range(slot_ref.shape[0] // 128):
        total = lax.fori_loop(k, code_ref.shape[0] // 128, functools.partial(block, k=k), jnp.zeros((8, 128), I32))
        row = jnp.sum(total.astype(F32), axis=0, keepdims=True) - 1.0
        slot_ref[k * 128:(k + 1) * 128, :] = column(row).astype(I32)


def gather_kernel(side, cap, lead, group, hid_hbm, head_hbm, ids_ref, valid_ref, acc,
                  hid, head, code_ref, pos_ref, slot_ref, pick, made, got, part, gat,
                  hid_sem, head_sem, made_sem, got_sem, ring_send, ring_recv, pair_send, pair_recv):
    chips = side * side
    devs = 2 * chips
    cols = made.shape[2]
    listed = gat.shape[1]
    half = listed // 2
    me = lax.axis_index('vocab')
    core = lax.rem(me, 2)
    chip = me // 2
    x, y = lax.rem(chip, side), chip // side

    def dev(a, b, c):
        px = lax.rem(x + a * (1 - c) + b * c, side)
        py = lax.rem(y + a * c + b * (1 - c), side)
        return (py * side + px) * 2 + c

    barrier = pltpu.get_barrier_semaphore()

    def greet(i, _):
        pl.semaphore_signal(barrier, inc=1, device_id={'vocab': lax.rem(me + i, devs)}, device_id_type=pl.DeviceIdType.MESH)
        return 0

    def turn(i):
        return lax.rem(chip + 1 + i, chips)

    def head_copy(q):
        return pltpu.make_async_copy(head_hbm.at[:, pl.ds(pl.multiple_of(q * 2 * cols, 2 * cols), 2 * cols)], head.at[q], head_sem.at[q])

    def head_start(i, _):
        head_copy(turn(i)).start()
        return 0

    lax.fori_loop(1, devs, greet, 0)
    lax.fori_loop(0, chips, head_start, 0)
    hid_copy = pltpu.make_async_copy(hid_hbm, hid, hid_sem)
    hid_copy.start()

    prepare(me, head.shape[1], cap, ids_ref, valid_ref, code_ref, pos_ref, pick)

    def make(i):
        q = turn(i)
        head_copy(q).wait()
        rows = jnp.dot(pick[...], head[q], preferred_element_type=F32).astype(BF16)
        made[2 * q] = rows[:, :cols]
        made[2 * q + 1] = rows[:, cols:]

    def give(d):
        return pltpu.make_async_remote_copy(
            src_ref=made.at[d], dst_ref=got.at[me], send_sem=made_sem.at[d], recv_sem=got_sem.at[me],
            device_id={'vocab': d}, device_id_type=pl.DeviceIdType.MESH)

    def give_chip(i):
        q = turn(i)
        give(2 * q).start()
        give(2 * q + 1).start()

    def make_give(i, _):
        make(i)

        @pl.when(i == lead)
        def _():
            pl.semaphore_wait(barrier, devs - 1)

        @pl.when(i >= lead)
        def _():
            give_chip(i - lead)

        return 0

    def give_only(i, _):
        give_chip(i)
        return 0

    lax.fori_loop(0, chips, make_give, 0)
    lax.fori_loop(chips - lead, chips - 1, give_only, 0)
    mate = chip * 2 + 1 - core
    compact(code_ref, pos_ref, slot_ref)
    part[...] = jnp.zeros_like(part)
    got[me] = made[me]
    give(mate).start()

    def got_wait(r):
        pltpu.make_async_remote_copy(
            src_ref=made.at[r], dst_ref=got.at[r], send_sem=made_sem.at[r], recv_sem=got_sem.at[r],
            device_id={'vocab': r}, device_id_type=pl.DeviceIdType.MESH).wait_recv()

    step = min(2 * cap, 256)
    band = math.gcd(256, listed)
    wide = listed // 2 if group > 1 else band

    def place(q):
        base = q * (2 * cap)
        pair = got[pl.ds(2 * q, 2)].reshape(2 * cap, cols)
        for k in range(2 * cap // step):
            slots = pair[k * step:(k + 1) * step]
            for m in range(listed // band):
                where = slot_ref[pl.ds(m * band, band), :] - base - k * step
                hot = []
                for c in range(0, step, 128):
                    w = min(128, step - c)
                    ids = lax.broadcasted_iota(I32, (band, 128), 1) + c
                    hot.append(jnp.where(where == ids, 1.0, 0.0).astype(BF16)[:, :w])
                hot = jnp.concatenate(hot, axis=1) if len(hot) > 1 else hot[0]
                part[pl.ds(m * band, band), :] += jnp.dot(hot, slots, preferred_element_type=F32)

    def place_step(i, _):
        q = lax.rem(chip + chips - 1 - i, chips)

        @pl.when(i < chips - 1)
        def _():
            got_wait(2 * q)
            got_wait(2 * q + 1)

        @pl.when(i == chips - 1)
        def _():
            got_wait(mate)

        place(q)
        return 0

    lax.fori_loop(0, chips, place_step, 0)
    gat[me] = part[...].astype(BF16)
    hid_copy.wait()
    acc[...] = jnp.zeros_like(acc)

    def piece(ref, d, h):
        return ref.at[d, pl.ds(h * half, half), :]

    def slot(a, b, h):
        return ((a % side) * side + (b % side)) * 2 + h

    sent = []

    def ring_copy(k, a, b, h, da, db):
        d = dev(a % side, b % side, core)
        to = dev(da % side, db % side, core)
        return pltpu.make_async_remote_copy(
            src_ref=piece(gat, d, h), dst_ref=piece(gat, d, h), send_sem=ring_send.at[k],
            recv_sem=ring_recv.at[slot(a - da, b - db, h)], device_id={'vocab': to}, device_id_type=pl.DeviceIdType.MESH)

    def ring(*at):
        ring_copy(len(sent), *at).start()
        sent.append(at)

    def pair_copy(a, b, h, c):
        d = dev(a % side, b % side, c)
        return pltpu.make_async_remote_copy(
            src_ref=piece(gat, d, h), dst_ref=piece(gat, d, h), send_sem=pair_send.at[slot(a, b, h)],
            recv_sem=pair_recv.at[slot(a, b, h)], device_id={'vocab': mate}, device_id_type=pl.DeviceIdType.MESH)

    def arrive(a, b, h):
        d = dev(a % side, b % side, core)
        pltpu.make_async_remote_copy(
            src_ref=piece(gat, d, h), dst_ref=piece(gat, d, h), send_sem=ring_send.at[0],
            recv_sem=ring_recv.at[slot(a, b, h)], device_id={'vocab': mate}, device_id_type=pl.DeviceIdType.MESH).wait_recv()

    def ready(a, b):
        for h in range(2):
            pair_copy(a, b, h, 1 - core).wait_recv()

    def add(slices):
        lhs = jnp.concatenate([hid[:, pl.ds(pl.multiple_of(d * cols, cols), cols)] for d in slices], axis=1)

        def columns(m, _):
            at = pl.ds(pl.multiple_of(m * wide, 128), wide)
            rhs = jnp.concatenate([gat[d, at, :] for d in slices], axis=1)
            acc[:, at] += lax.dot_general(lhs, rhs, (((1,), (1,)), ((), ())), preferred_element_type=F32)
            return 0

        lax.fori_loop(0, listed // wide, columns, 0)

    far = side // 2

    def take(a, b, h):
        if (a, b) != (0, 0):
            arrive(a, b, h)
        if b == 0:
            if a == 0:
                order = (-1, 1) if h == 0 else (1, -1)
                for s in order:
                    ring(a, b, h, s, 0)
            elif a == 1 and h == 0:
                ring(a, b, h, -1, 0)
            elif a == -1 and h == 1:
                ring(a, b, h, 1, 0)
            for s in (-1, 1):
                ring(a, b, h, 0, s)
        elif b == 1 and h == 0:
            ring(a, b, h, 0, -1)
        elif b == -1 and h == 1:
            ring(a, b, h, 0, 1)
        pair_copy(a, b, h, core).start()

    for s, h in ((-1, 0), (1, 1)):
        ring(0, 0, h, s, 0)
        ring(0, 0, h, 0, s)
    for h in range(2):
        pair_copy(0, 0, h, core).start()
    for s, h in ((-1, 1), (1, 0)):
        ring(0, 0, h, s, 0)
        ring(0, 0, h, 0, s)

    phases = [
        ([(1, 0, 0), (-1, 0, 1), (0, 1, 0), (0, -1, 1), (1, 0, 1), (-1, 0, 0), (0, 1, 1), (0, -1, 0)], [(0, 0), (1, 0)]),
        ([], [(-1, 0), (0, 1)]),
        ([(far, 0, 0), (far, 0, 1)], [(0, -1), (far, 0)]),
        ([(1, 1, 0), (-1, -1, 1), (-1, 1, 0), (1, -1, 1), (0, far, 0), (0, far, 1), (1, 1, 1), (-1, -1, 0)], [(0, far), (1, 1)]),
        ([(-1, 1, 1), (1, -1, 0), (far, 1, 0), (far, -1, 1)], [(-1, -1), (-1, 1)]),
        ([(far, 1, 1), (far, -1, 0), (1, far, 0), (1, far, 1)], [(1, -1), (far, 1)]),
        ([(-1, far, 0), (-1, far, 1)], [(far, -1), (1, far)]),
        ([(far, far, 0), (far, far, 1)], [(-1, far), (far, far)]),
    ]

    def phase(p, _):
        at = [0] * 4
        for k, (takes, adds) in enumerate(phases):
            @pl.when(p == k)
            def _():
                for t in takes:
                    take(*t)
                for t in adds:
                    ready(*t)
            for i, v in enumerate(sum(adds, ())):
                at[i] = at[i] + (p == k).astype(I32) * (v % side)
        slices = [dev(at[0], at[1], core), dev(at[0], at[1], 1 - core), dev(at[2], at[3], core), dev(at[2], at[3], 1 - core)]
        for g in range(0, 4, 2 * group):
            add(slices[g:g + 2 * group])
        return 0

    lax.fori_loop(0, len(phases), phase, 0)

    for k, at in enumerate(sent):
        ring_copy(k, *at).wait_send()
    for a in range(side):
        for b in range(side):
            for h in range(2):
                pair_copy(a, b, h, core).wait_send()

    def given(i, _):
        give(lax.rem(me + i, devs)).wait_send()
        return 0

    lax.fori_loop(1, devs, given, 0)


def gather_scores(shards, listed, cap, group, collective_id, hidden, w_head, ids, valid):
    rows, depth = hidden.shape
    n = ids.shape[0] * ids.shape[1]
    vocab_local = w_head.shape[0]
    cols = depth // shards
    side = math.isqrt(shards // 2)
    vmem = pl.BlockSpec(memory_space=pltpu.VMEM)
    hbm = pl.BlockSpec(memory_space=pl.ANY)
    dma = pltpu.SemaphoreType.DMA
    limit = 2 * (rows * depth + vocab_local * depth + cap * (vocab_local + 2 * depth) + listed * depth + 4 * (n + listed) * cols) + 10 * 1024 * 1024
    return pl.pallas_call(
        functools.partial(gather_kernel, side, cap, LEAD, group),
        out_shape=jax.ShapeDtypeStruct((rows, listed), F32),
        in_specs=[hbm, hbm, vmem, vmem],
        out_specs=vmem,
        scratch_shapes=[
            pltpu.VMEM((rows, depth), BF16),
            pltpu.VMEM((shards // 2, vocab_local, 2 * cols), BF16),
            pltpu.VMEM((n, 128), I32),
            pltpu.VMEM((n, 128), I32),
            pltpu.VMEM((listed, 128), I32),
            pltpu.VMEM((cap, vocab_local), BF16),
            pltpu.VMEM((shards, cap, cols), BF16),
            pltpu.VMEM((shards, cap, cols), BF16),
            pltpu.VMEM((listed, cols), F32),
            pltpu.VMEM((shards, listed, cols), BF16),
            dma, dma((shards // 2,)), dma((shards,)), dma((shards,)),
            dma((30,)), dma((shards,)), dma((shards,)), dma((shards,)),
        ],
        compiler_params=pltpu.CompilerParams(collective_id=collective_id, has_side_effects=True, vmem_limit_bytes=limit),
        name=f'gather_scores_{listed}_{cap}',
    )(hidden, w_head, ids, valid)


def finish_kernel(band, score_ref, valid_ref, target_ref, probs_ref, logp_ref, wide, cols_ref, place_ref, local_ref):
    rows, n = probs_ref.shape
    listed = score_ref.shape[1]
    chunks = n // 128

    @pl.when(pl.program_id(0) == 0)
    def _():
        flags = valid_ref[...].astype(F32)
        upper = (lax.broadcasted_iota(I32, (128, 128), 0) < lane_ids(128)).astype(F32).astype(BF16)
        inner = jnp.dot(flags.astype(BF16), upper, preferred_element_type=F32)
        totals = jnp.broadcast_to(jnp.sum(flags, axis=1, keepdims=True), (chunks, 128))
        above = (lax.broadcasted_iota(I32, (chunks, chunks), 0) > lax.broadcasted_iota(I32, (chunks, chunks), 1)).astype(F32)
        base = jnp.dot(above.astype(BF16), totals.astype(BF16), preferred_element_type=F32).astype(I32)
        local_ref[...] = inner.astype(I32) + (base & 127)
        for c in range(chunks):
            place_ref[c] = base[c, 0] >> 7
        wide[:, listed:] = jnp.zeros((wide.shape[0], wide.shape[1] - listed), F32)

    first = pl.program_id(0) * rows
    cols_ref[...] = column(target_ref[0].astype(F32))[:rows]

    def some(r, _):
        at = pl.ds(pl.multiple_of(r * band, band), band)
        wide[:, :listed] = score_ref[pl.ds(pl.multiple_of(first + r * band, band), band), :] * INV_TEMP
        target = cols_ref[at, :].astype(I32)
        top = jnp.full((band, 128), -jnp.inf, F32)
        picked = jnp.zeros((band, 128), F32)
        for c in range(chunks):
            begin = place_ref[c] * 128
            local = jnp.broadcast_to(local_ref[c:c + 1, :], (band, 128))
            lower = jnp.take_along_axis(wide[:, pl.ds(pl.multiple_of(begin, 128), 128)], local & 127, axis=1, mode='promise_in_bounds')
            upper = jnp.take_along_axis(wide[:, pl.ds(pl.multiple_of(begin + 128, 128), 128)], local & 127, axis=1, mode='promise_in_bounds')
            part = jnp.where(local < 128, lower, upper)
            probs_ref[at, c * 128:(c + 1) * 128] = part
            top = jnp.maximum(top, jnp.where(valid_ref[c:c + 1, :] > 0, part, -jnp.inf))
            picked += jnp.where(target == lane_ids(band) + c * 128, part, 0.0)
        top = jnp.max(top, axis=1, keepdims=True)
        total = jnp.zeros((band, 128), F32)
        for c in range(chunks):
            terms = jnp.where(valid_ref[c:c + 1, :] > 0, jnp.exp(probs_ref[at, c * 128:(c + 1) * 128] - top), 0.0)
            probs_ref[at, c * 128:(c + 1) * 128] = terms
            total += terms
        total = jnp.sum(total, axis=1, keepdims=True)
        probs_ref[at, :] = probs_ref[at, :] * (1.0 / total)
        logp = jnp.sum(picked, axis=1, keepdims=True) - (top + jnp.log(total))
        cols_ref[at, :] = jnp.broadcast_to(logp, (band, 128))
        return 0

    lax.fori_loop(0, rows // band, some, 0)
    logp_ref[0] = jnp.transpose(cols_ref[...])[:1]


def finish(scores, valid, target_pos, band):
    rows, listed = scores.shape
    n = valid.shape[0] * valid.shape[1]
    block = min(128, rows)
    band = min(band, block)
    probs, logp = pl.pallas_call(
        functools.partial(finish_kernel, band),
        grid=(rows // block,),
        out_shape=(jax.ShapeDtypeStruct((rows, n), F32), jax.ShapeDtypeStruct((rows // block, 1, block), F32)),
        in_specs=[pl.BlockSpec(memory_space=pltpu.VMEM), pl.BlockSpec(valid.shape, lambda i: (0, 0)),
                  pl.BlockSpec((1, 1, block), lambda i: (i, 0, 0))],
        out_specs=(pl.BlockSpec((block, n), lambda i: (i, 0)), pl.BlockSpec((1, 1, block), lambda i: (i, 0, 0))),
        scratch_shapes=[pltpu.VMEM((band, listed + 256), F32), pltpu.VMEM((block, 128), F32), pltpu.SMEM((n // 128,), I32), pltpu.VMEM((n // 128, 128), I32)],
        compiler_params=pltpu.CompilerParams(dimension_semantics=('arbitrary',), vmem_limit_bytes=16 * 1024 * 1024),
        name='finish',
    )(scores, valid, target_pos.reshape(rows // block, 1, block))
    return probs, logp.reshape(rows)


def plans(n, shards, vocab_local):
    mean = 2 * n // shards
    sizes = [-(-n * i // 1024) * 128 for i in SIZES]
    caps = [min(mean, -(-(mean * size * 23 // (20 * n)) // 16) * 16) for size in sizes]
    return list(zip(sizes, caps)) + [(n, vocab_local)]


def solution(mesh):
    shards = mesh.shape['vocab']

    def device_step(hidden, w_head, allowed_ids, allowed_valid, target_pos):
        vocab_local = w_head.shape[0]
        n = allowed_ids.shape[0]
        owner = power_div(allowed_ids, vocab_local)
        counts = jnp.sum((owner[None, :] == jnp.arange(shards)[:, None]) & (allowed_valid > 0)[None, :], axis=1, dtype=I32)
        most, every = jnp.max(counts), jnp.sum(counts)
        choice = jnp.int32(0)
        runs = []
        for i, (size, cap) in enumerate(plans(n, shards, vocab_local)):
            group = 1 if cap == vocab_local else 2

            def run(hidden, w_head, ids, valid, target, size=size, cap=cap, group=group, i=i):
                return finish(gather_scores(shards, size, cap, group, i, hidden, w_head, ids, valid), valid, target, 32 if group == 1 else 128)

            runs.append(run)
            if cap < vocab_local:
                choice += jnp.where((every <= size) & (most <= cap), 0, 1)
        square = (n // 128, 128)
        return lax.switch(choice, runs, hidden, w_head, allowed_ids.reshape(square), allowed_valid.reshape(square), target_pos)

    row_spec = P(('rep', 'vocab'))
    mat_spec = P(('rep', 'vocab'), None)
    return jax.shard_map(device_step, mesh=mesh, in_specs=(mat_spec, P('vocab', None), P('rep'), P('rep'), row_spec), out_specs=(mat_spec, row_spec), check_vma=False)
```

```python
import functools
import math

import jax
import jax.numpy as jnp
from jax import lax
from jax.experimental import pallas as pl
from jax.experimental.pallas import tpu as pltpu
from jax.sharding import PartitionSpec as P

INV_TEMP = 1.25
SIZES = (5, 6, 7, 8)
SPARE = 16
LEAD = 2
F32, BF16, I32 = jnp.float32, jnp.bfloat16, jnp.int32


def column(row):
    return jnp.transpose(jnp.broadcast_to(row, (128, 128)))


def lane_ids(rows):
    return lax.broadcasted_iota(I32, (rows, 128), 1)


def power_div(value, by):
    return value >> (by.bit_length() - 1) if by & (by - 1) == 0 else value // by


def prepare(me, vocab_local, cap, ids_ref, valid_ref, code_ref, pos_ref, pick):
    lanes = lane_ids(128)
    below = (lax.broadcasted_iota(I32, (128, 128), 0) > lanes).astype(F32).astype(BF16)
    before = jnp.zeros((1, 128), F32)
    mine = [jnp.zeros((1, 128), F32) for _ in range(-(-cap // 128))]
    for b in range(ids_ref.shape[0]):
        ids = jnp.where(valid_ref[b:b + 1, :] > 0, ids_ref[b:b + 1, :], -1)
        ids = column(ids.astype(F32)).astype(I32)
        valid = ids >= 0
        owner = jnp.where(valid, power_div(ids, vocab_local), -1)
        own = (owner == lanes).astype(F32)
        hot = jnp.where((lanes == 127) & valid, 1.0, own)
        number = jnp.dot(below, hot.astype(BF16), preferred_element_type=F32) + before
        before = before + jnp.sum(hot, axis=0, keepdims=True)
        pos = jnp.sum(jnp.where(lanes == 127, number, 0.0), axis=1, keepdims=True).astype(I32)
        number = jnp.sum(own * number, axis=1, keepdims=True).astype(I32)
        code = jnp.where(valid, owner * cap + number, -1)
        code_ref[b * 128:(b + 1) * 128, :] = code
        pos_ref[b * 128:(b + 1) * 128, :] = jnp.where(valid, pos, -1)
        local = (ids - me * vocab_local + 1).astype(F32)
        for c in range(len(mine)):
            mine[c] += jnp.sum(jnp.where(code == lanes + (me * cap + c * 128), local, 0.0), axis=0, keepdims=True)
    for c in range(len(mine)):
        rows = min(128, cap - c * 128)
        local = (column(mine[c]) - 1.0).astype(I32)[:rows]
        for k in range(0, vocab_local, 128):
            pick[c * 128:c * 128 + rows, k:k + 128] = (local == lane_ids(rows) + k).astype(F32).astype(BF16)


def compact(code_ref, pos_ref, slot_ref):
    def block(b, total, k):
        at = pl.ds(pl.multiple_of(b * 128, 128), 128)
        here = jnp.where(pos_ref[at, :] == lane_ids(128) + k * 128, code_ref[at, :] + 1, 0)
        return total + jnp.sum(here.reshape(16, 8, 128), axis=0)

    for k in range(slot_ref.shape[0] // 128):
        total = lax.fori_loop(k, code_ref.shape[0] // 128, functools.partial(block, k=k), jnp.zeros((8, 128), I32))
        row = jnp.sum(total.astype(F32), axis=0, keepdims=True) - 1.0
        slot_ref[k * 128:(k + 1) * 128, :] = column(row).astype(I32)


def gather_kernel(side, cap, lead, group, hid_hbm, head_hbm, ids_ref, valid_ref, acc,
                  hid, head, code_ref, pos_ref, slot_ref, pick, made, got, part, gat,
                  hid_sem, head_sem, made_sem, got_sem, ring_send, ring_recv, pair_send, pair_recv):
    chips = side * side
    devs = 2 * chips
    cols = made.shape[2]
    listed = gat.shape[1]
    half = listed // 2
    me = lax.axis_index('vocab')
    core = lax.rem(me, 2)
    chip = me // 2
    x, y = lax.rem(chip, side), chip // side

    def dev(a, b, c):
        px = lax.rem(x + a * (1 - c) + b * c, side)
        py = lax.rem(y + a * c + b * (1 - c), side)
        return (py * side + px) * 2 + c

    barrier = pltpu.get_barrier_semaphore()

    def greet(i, _):
        pl.semaphore_signal(barrier, inc=1, device_id={'vocab': lax.rem(me + i, devs)}, device_id_type=pl.DeviceIdType.MESH)
        return 0

    def turn(i):
        return lax.rem(chip + 1 + i, chips)

    def head_copy(q):
        return pltpu.make_async_copy(head_hbm.at[:, pl.ds(pl.multiple_of(q * 2 * cols, 2 * cols), 2 * cols)], head.at[q], head_sem.at[q])

    def head_start(i, _):
        head_copy(turn(i)).start()
        return 0

    lax.fori_loop(1, devs, greet, 0)
    lax.fori_loop(0, chips, head_start, 0)
    hid_copy = pltpu.make_async_copy(hid_hbm, hid, hid_sem)
    hid_copy.start()

    prepare(me, head.shape[1], cap, ids_ref, valid_ref, code_ref, pos_ref, pick)

    def make(i):
        q = turn(i)
        head_copy(q).wait()
        rows = jnp.dot(pick[...], head[q], preferred_element_type=F32).astype(BF16)
        made[2 * q] = rows[:, :cols]
        made[2 * q + 1] = rows[:, cols:]

    def give(d):
        return pltpu.make_async_remote_copy(
            src_ref=made.at[d], dst_ref=got.at[me], send_sem=made_sem.at[d], recv_sem=got_sem.at[me],
            device_id={'vocab': d}, device_id_type=pl.DeviceIdType.MESH)

    def give_chip(i):
        q = turn(i)
        give(2 * q).start()
        give(2 * q + 1).start()

    def make_give(i, _):
        make(i)

        @pl.when(i == lead)
        def _():
            pl.semaphore_wait(barrier, devs - 1)

        @pl.when(i >= lead)
        def _():
            give_chip(i - lead)

        return 0

    def give_only(i, _):
        give_chip(i)
        return 0

    lax.fori_loop(0, chips, make_give, 0)
    lax.fori_loop(chips - lead, chips - 1, give_only, 0)
    mate = chip * 2 + 1 - core
    compact(code_ref, pos_ref, slot_ref)
    part[...] = jnp.zeros_like(part)
    got[me] = made[me]
    give(mate).start()

    def got_wait(r):
        pltpu.make_async_remote_copy(
            src_ref=made.at[r], dst_ref=got.at[r], send_sem=made_sem.at[r], recv_sem=got_sem.at[r],
            device_id={'vocab': r}, device_id_type=pl.DeviceIdType.MESH).wait_recv()

    step = min(2 * cap, 256)
    band = math.gcd(256, listed)
    wide = listed // 2 if group > 1 else band

    def place(q):
        base = q * (2 * cap)
        pair = got[pl.ds(2 * q, 2)].reshape(2 * cap, cols)
        for k in range(2 * cap // step):
            slots = pair[k * step:(k + 1) * step]
            for m in range(listed // band):
                where = slot_ref[pl.ds(m * band, band), :] - base - k * step
                hot = []
                for c in range(0, step, 128):
                    w = min(128, step - c)
                    ids = lax.broadcasted_iota(I32, (band, 128), 1) + c
                    hot.append(jnp.where(where == ids, 1.0, 0.0).astype(BF16)[:, :w])
                hot = jnp.concatenate(hot, axis=1) if len(hot) > 1 else hot[0]
                part[pl.ds(m * band, band), :] += jnp.dot(hot, slots, preferred_element_type=F32)

    def place_step(i, _):
        q = lax.rem(chip + chips - 1 - i, chips)

        @pl.when(i < chips - 1)
        def _():
            got_wait(2 * q)
            got_wait(2 * q + 1)

        @pl.when(i == chips - 1)
        def _():
            got_wait(mate)

        place(q)
        return 0

    lax.fori_loop(0, chips, place_step, 0)
    gat[me] = part[...].astype(BF16)
    hid_copy.wait()
    acc[...] = jnp.zeros_like(acc)

    def piece(ref, d, h):
        return ref.at[d, pl.ds(h * half, half), :]

    def slot(a, b, h):
        return ((a % side) * side + (b % side)) * 2 + h

    sent = []

    def ring_copy(k, a, b, h, da, db):
        d = dev(a % side, b % side, core)
        to = dev(da % side, db % side, core)
        return pltpu.make_async_remote_copy(
            src_ref=piece(gat, d, h), dst_ref=piece(gat, d, h), send_sem=ring_send.at[k],
            recv_sem=ring_recv.at[slot(a - da, b - db, h)], device_id={'vocab': to}, device_id_type=pl.DeviceIdType.MESH)

    def ring(*at):
        ring_copy(len(sent), *at).start()
        sent.append(at)

    def pair_copy(a, b, h, c):
        d = dev(a % side, b % side, c)
        return pltpu.make_async_remote_copy(
            src_ref=piece(gat, d, h), dst_ref=piece(gat, d, h), send_sem=pair_send.at[slot(a, b, h)],
            recv_sem=pair_recv.at[slot(a, b, h)], device_id={'vocab': mate}, device_id_type=pl.DeviceIdType.MESH)

    def arrive(a, b, h):
        d = dev(a % side, b % side, core)
        pltpu.make_async_remote_copy(
            src_ref=piece(gat, d, h), dst_ref=piece(gat, d, h), send_sem=ring_send.at[0],
            recv_sem=ring_recv.at[slot(a, b, h)], device_id={'vocab': mate}, device_id_type=pl.DeviceIdType.MESH).wait_recv()

    def ready(a, b):
        for h in range(2):
            pair_copy(a, b, h, 1 - core).wait_recv()

    def add(slices):
        lhs = jnp.concatenate([hid[:, pl.ds(pl.multiple_of(d * cols, cols), cols)] for d in slices], axis=1)

        def columns(m, _):
            at = pl.ds(pl.multiple_of(m * wide, 128), wide)
            rhs = jnp.concatenate([gat[d, at, :] for d in slices], axis=1)
            acc[:, at] += lax.dot_general(lhs, rhs, (((1,), (1,)), ((), ())), preferred_element_type=F32)
            return 0

        lax.fori_loop(0, listed // wide, columns, 0)

    far = side // 2

    def take(a, b, h):
        if (a, b) != (0, 0):
            arrive(a, b, h)
        if b == 0:
            if a == 0:
                order = (-1, 1) if h == 0 else (1, -1)
                for s in order:
                    ring(a, b, h, s, 0)
            elif a == 1 and h == 0:
                ring(a, b, h, -1, 0)
            elif a == -1 and h == 1:
                ring(a, b, h, 1, 0)
            for s in (-1, 1):
                ring(a, b, h, 0, s)
        elif b == 1 and h == 0:
            ring(a, b, h, 0, -1)
        elif b == -1 and h == 1:
            ring(a, b, h, 0, 1)
        pair_copy(a, b, h, core).start()

    for s, h in ((-1, 0), (1, 1)):
        ring(0, 0, h, s, 0)
        ring(0, 0, h, 0, s)
    for h in range(2):
        pair_copy(0, 0, h, core).start()
    for s, h in ((-1, 1), (1, 0)):
        ring(0, 0, h, s, 0)
        ring(0, 0, h, 0, s)

    phases = [
        ([(1, 0, 0), (-1, 0, 1), (0, 1, 0), (0, -1, 1), (1, 0, 1), (-1, 0, 0), (0, 1, 1), (0, -1, 0)], [(0, 0), (1, 0)]),
        ([], [(-1, 0), (0, 1)]),
        ([(far, 0, 0), (far, 0, 1)], [(0, -1), (far, 0)]),
        ([(1, 1, 0), (-1, -1, 1), (-1, 1, 0), (1, -1, 1), (0, far, 0), (0, far, 1), (1, 1, 1), (-1, -1, 0)], [(0, far), (1, 1)]),
        ([(-1, 1, 1), (1, -1, 0), (far, 1, 0), (far, -1, 1)], [(-1, -1), (-1, 1)]),
        ([(far, 1, 1), (far, -1, 0), (1, far, 0), (1, far, 1)], [(1, -1), (far, 1)]),
        ([(-1, far, 0), (-1, far, 1)], [(far, -1), (1, far)]),
        ([(far, far, 0), (far, far, 1)], [(-1, far), (far, far)]),
    ]

    def phase(p, _):
        at = [0] * 4
        for k, (takes, adds) in enumerate(phases):
            @pl.when(p == k)
            def _():
                for t in takes:
                    take(*t)
                for t in adds:
                    ready(*t)
            for i, v in enumerate(sum(adds, ())):
                at[i] = at[i] + (p == k).astype(I32) * (v % side)
        slices = [dev(at[0], at[1], core), dev(at[0], at[1], 1 - core), dev(at[2], at[3], core), dev(at[2], at[3], 1 - core)]
        for g in range(0, 4, 2 * group):
            add(slices[g:g + 2 * group])
        return 0

    lax.fori_loop(0, len(phases), phase, 0)

    for k, at in enumerate(sent):
        ring_copy(k, *at).wait_send()
    for a in range(side):
        for b in range(side):
            for h in range(2):
                pair_copy(a, b, h, core).wait_send()

    def given(i, _):
        give(lax.rem(me + i, devs)).wait_send()
        return 0

    lax.fori_loop(1, devs, given, 0)


def gather_scores(shards, listed, cap, group, collective_id, hidden, w_head, ids, valid):
    rows, depth = hidden.shape
    n = ids.shape[0] * ids.shape[1]
    vocab_local = w_head.shape[0]
    cols = depth // shards
    side = math.isqrt(shards // 2)
    vmem = pl.BlockSpec(memory_space=pltpu.VMEM)
    hbm = pl.BlockSpec(memory_space=pl.ANY)
    dma = pltpu.SemaphoreType.DMA
    limit = 2 * (rows * depth + vocab_local * depth + cap * (vocab_local + 2 * depth) + listed * depth + 4 * (n + listed) * cols) + 10 * 1024 * 1024
    return pl.pallas_call(
        functools.partial(gather_kernel, side, cap, LEAD, group),
        out_shape=jax.ShapeDtypeStruct((rows, listed), F32),
        in_specs=[hbm, hbm, vmem, vmem],
        out_specs=vmem,
        scratch_shapes=[
            pltpu.VMEM((rows, depth), BF16),
            pltpu.VMEM((shards // 2, vocab_local, 2 * cols), BF16),
            pltpu.VMEM((n, 128), I32),
            pltpu.VMEM((n, 128), I32),
            pltpu.VMEM((listed, 128), I32),
            pltpu.VMEM((cap, vocab_local), BF16),
            pltpu.VMEM((shards, cap, cols), BF16),
            pltpu.VMEM((shards, cap, cols), BF16),
            pltpu.VMEM((listed, cols), F32),
            pltpu.VMEM((shards, listed, cols), BF16),
            dma, dma((shards // 2,)), dma((shards,)), dma((shards,)),
            dma((30,)), dma((shards,)), dma((shards,)), dma((shards,)),
        ],
        compiler_params=pltpu.CompilerParams(collective_id=collective_id, has_side_effects=True, vmem_limit_bytes=limit),
        name=f'gather_scores_{listed}_{cap}',
    )(hidden, w_head, ids, valid)


def finish_kernel(band, score_ref, valid_ref, target_ref, probs_ref, logp_ref, wide, cols_ref, place_ref, local_ref):
    rows, n = probs_ref.shape
    listed = score_ref.shape[1]
    chunks = n // 128

    @pl.when(pl.program_id(0) == 0)
    def _():
        flags = valid_ref[...].astype(F32)
        upper = (lax.broadcasted_iota(I32, (128, 128), 0) < lane_ids(128)).astype(F32).astype(BF16)
        inner = jnp.dot(flags.astype(BF16), upper, preferred_element_type=F32)
        totals = jnp.broadcast_to(jnp.sum(flags, axis=1, keepdims=True), (chunks, 128))
        above = (lax.broadcasted_iota(I32, (chunks, chunks), 0) > lax.broadcasted_iota(I32, (chunks, chunks), 1)).astype(F32)
        base = jnp.dot(above.astype(BF16), totals.astype(BF16), preferred_element_type=F32).astype(I32)
        local_ref[...] = inner.astype(I32) + (base & 127)
        for c in range(chunks):
            place_ref[c] = base[c, 0] >> 7
        wide[:, listed:] = jnp.zeros((wide.shape[0], wide.shape[1] - listed), F32)

    first = pl.program_id(0) * rows
    cols_ref[...] = column(target_ref[0].astype(F32))[:rows]

    def some(r, _):
        at = pl.ds(pl.multiple_of(r * band, band), band)
        wide[:, :listed] = score_ref[pl.ds(pl.multiple_of(first + r * band, band), band), :] * INV_TEMP
        target = cols_ref[at, :].astype(I32)
        top = jnp.full((band, 128), -jnp.inf, F32)
        picked = jnp.zeros((band, 128), F32)
        for c in range(chunks):
            begin = place_ref[c] * 128
            local = jnp.broadcast_to(local_ref[c:c + 1, :], (band, 128))
            lower = jnp.take_along_axis(wide[:, pl.ds(pl.multiple_of(begin, 128), 128)], local & 127, axis=1, mode='promise_in_bounds')
            upper = jnp.take_along_axis(wide[:, pl.ds(pl.multiple_of(begin + 128, 128), 128)], local & 127, axis=1, mode='promise_in_bounds')
            part = jnp.where(local < 128, lower, upper)
            probs_ref[at, c * 128:(c + 1) * 128] = part
            top = jnp.maximum(top, jnp.where(valid_ref[c:c + 1, :] > 0, part, -jnp.inf))
            picked += jnp.where(target == lane_ids(band) + c * 128, part, 0.0)
        top = jnp.max(top, axis=1, keepdims=True)
        total = jnp.zeros((band, 128), F32)
        for c in range(chunks):
            terms = jnp.where(valid_ref[c:c + 1, :] > 0, jnp.exp(probs_ref[at, c * 128:(c + 1) * 128] - top), 0.0)
            probs_ref[at, c * 128:(c + 1) * 128] = terms
            total += terms
        total = jnp.sum(total, axis=1, keepdims=True)
        probs_ref[at, :] = probs_ref[at, :] * (1.0 / total)
        logp = jnp.sum(picked, axis=1, keepdims=True) - (top + jnp.log(total))
        cols_ref[at, :] = jnp.broadcast_to(logp, (band, 128))
        return 0

    lax.fori_loop(0, rows // band, some, 0)
    logp_ref[0] = jnp.transpose(cols_ref[...])[:1]


def finish(scores, valid, target_pos, band):
    rows, listed = scores.shape
    n = valid.shape[0] * valid.shape[1]
    block = min(128, rows)
    band = min(band, block)
    probs, logp = pl.pallas_call(
        functools.partial(finish_kernel, band),
        grid=(rows // block,),
        out_shape=(jax.ShapeDtypeStruct((rows, n), F32), jax.ShapeDtypeStruct((rows // block, 1, block), F32)),
        in_specs=[pl.BlockSpec(memory_space=pltpu.VMEM), pl.BlockSpec(valid.shape, lambda i: (0, 0)),
                  pl.BlockSpec((1, 1, block), lambda i: (i, 0, 0))],
        out_specs=(pl.BlockSpec((block, n), lambda i: (i, 0)), pl.BlockSpec((1, 1, block), lambda i: (i, 0, 0))),
        scratch_shapes=[pltpu.VMEM((band, listed + 256), F32), pltpu.VMEM((block, 128), F32), pltpu.SMEM((n // 128,), I32), pltpu.VMEM((n // 128, 128), I32)],
        compiler_params=pltpu.CompilerParams(dimension_semantics=('arbitrary',), vmem_limit_bytes=16 * 1024 * 1024),
        name='finish',
    )(scores, valid, target_pos.reshape(rows // block, 1, block))
    return probs, logp.reshape(rows)


def choose_kernel(shards, vocab_local, fits, ids_ref, valid_ref, choice_ref):
    owner = jnp.where(valid_ref[...] > 0, power_div(ids_ref[...], vocab_local), -1)
    counts = [jnp.sum((owner == r).astype(F32), axis=0, keepdims=True) for r in range(shards)]
    counts = jnp.sum(jnp.concatenate(counts, axis=0), axis=1, keepdims=True)
    most, every = jnp.max(counts), jnp.sum(counts)
    choice = jnp.int32(0)
    for size, cap in fits:
        choice += jnp.where((every <= float(size)) & (most <= float(cap)), jnp.int32(0), jnp.int32(1))
    choice_ref[0] = choice


def choose(shards, vocab_local, fits, ids, valid):
    return pl.pallas_call(
        functools.partial(choose_kernel, shards, vocab_local, fits),
        out_shape=jax.ShapeDtypeStruct((1,), I32),
        in_specs=[pl.BlockSpec(memory_space=pltpu.VMEM)] * 2,
        out_specs=pl.BlockSpec(memory_space=pltpu.SMEM),
        compiler_params=pltpu.CompilerParams(vmem_limit_bytes=1024 * 1024),
        name='choose',
    )(ids, valid)[0]


def plans(n, shards, vocab_local):
    mean = 2 * n // shards
    sizes = [-(-n * i // 1024) * 128 for i in SIZES]
    caps = [min(mean, -(-(mean * size // n + mean // SPARE) // 8) * 8) for size in sizes]
    return list(zip(sizes, caps)) + [(n, vocab_local)]


def solution(mesh):
    shards = mesh.shape['vocab']

    def device_step(hidden, w_head, allowed_ids, allowed_valid, target_pos):
        vocab_local = w_head.shape[0]
        n = allowed_ids.shape[0]
        runs = []
        for i, (size, cap) in enumerate(plans(n, shards, vocab_local)):
            group = 1 if cap == vocab_local else 2

            def run(hidden, w_head, ids, valid, target, size=size, cap=cap, group=group, i=i):
                return finish(gather_scores(shards, size, cap, group, i, hidden, w_head, ids, valid), valid, target, 32 if group == 1 else 128)

            runs.append(run)
        ids, valid = allowed_ids.reshape(n // 128, 128), allowed_valid.reshape(n // 128, 128)
        choice = choose(shards, vocab_local, plans(n, shards, vocab_local)[:-1], ids, valid)
        return lax.switch(choice, runs, hidden, w_head, ids, valid, target_pos)

    row_spec = P(('rep', 'vocab'))
    mat_spec = P(('rep', 'vocab'), None)
    return jax.shard_map(device_step, mesh=mesh, in_specs=(mat_spec, P('vocab', None), P('rep'), P('rep'), row_spec), out_specs=(mat_spec, row_spec), check_vma=False)
```

```python
import functools
import math

import jax
import jax.numpy as jnp
from jax import lax
from jax.experimental import pallas as pl
from jax.experimental.pallas import tpu as pltpu
from jax.sharding import PartitionSpec as P

INV_TEMP = 1.25
SIZES = (5, 6, 7, 8)
SPARE = 16
EARLY = 2
LEAD = 2
F32, BF16, I32 = jnp.float32, jnp.bfloat16, jnp.int32


def column(row):
    return jnp.transpose(jnp.broadcast_to(row, (128, 128)))


def lane_ids(rows):
    return lax.broadcasted_iota(I32, (rows, 128), 1)


def power_div(value, by):
    return value >> (by.bit_length() - 1) if by & (by - 1) == 0 else value // by


def prepare(me, vocab_local, cap, ids_ref, valid_ref, code_ref, pos_ref, pick):
    lanes = lane_ids(128)
    below = (lax.broadcasted_iota(I32, (128, 128), 0) > lanes).astype(F32).astype(BF16)
    before = jnp.zeros((1, 128), F32)
    mine = [jnp.zeros((1, 128), F32) for _ in range(-(-cap // 128))]
    for b in range(ids_ref.shape[0]):
        ids = jnp.where(valid_ref[b:b + 1, :] > 0, ids_ref[b:b + 1, :], -1)
        ids = column(ids.astype(F32)).astype(I32)
        valid = ids >= 0
        owner = jnp.where(valid, power_div(ids, vocab_local), -1)
        own = (owner == lanes).astype(F32)
        hot = jnp.where((lanes == 127) & valid, 1.0, own)
        number = jnp.dot(below, hot.astype(BF16), preferred_element_type=F32) + before
        before = before + jnp.sum(hot, axis=0, keepdims=True)
        pos = jnp.sum(jnp.where(lanes == 127, number, 0.0), axis=1, keepdims=True).astype(I32)
        number = jnp.sum(own * number, axis=1, keepdims=True).astype(I32)
        code = jnp.where(valid, owner * cap + number, -1)
        code_ref[b * 128:(b + 1) * 128, :] = code
        pos_ref[b * 128:(b + 1) * 128, :] = jnp.where(valid, pos, -1)
        local = (ids - me * vocab_local + 1).astype(F32)
        for c in range(len(mine)):
            mine[c] += jnp.sum(jnp.where(code == lanes + (me * cap + c * 128), local, 0.0), axis=0, keepdims=True)
    for c in range(len(mine)):
        rows = min(128, cap - c * 128)
        local = (column(mine[c]) - 1.0).astype(I32)[:rows]
        for k in range(0, vocab_local, 128):
            pick[c * 128:c * 128 + rows, k:k + 128] = (local == lane_ids(rows) + k).astype(F32).astype(BF16)


def compact(code_ref, pos_ref, slot_ref):
    def block(b, total, k):
        at = pl.ds(pl.multiple_of(b * 128, 128), 128)
        here = jnp.where(pos_ref[at, :] == lane_ids(128) + k * 128, code_ref[at, :] + 1, 0)
        return total + jnp.sum(here.reshape(16, 8, 128), axis=0)

    for k in range(slot_ref.shape[0] // 128):
        total = lax.fori_loop(k, code_ref.shape[0] // 128, functools.partial(block, k=k), jnp.zeros((8, 128), I32))
        row = jnp.sum(total.astype(F32), axis=0, keepdims=True) - 1.0
        slot_ref[k * 128:(k + 1) * 128, :] = column(row).astype(I32)


def gather_kernel(side, cap, lead, compact_code, hid_hbm, head_hbm, ids_ref, valid_ref, acc,
                  hid, head, code_ref, pos_ref, slot_ref, pick, made, got, part, gat,
                  hid_sem, head_sem, made_sem, got_sem, ring_send, ring_recv, pair_send, pair_recv):
    chips = side * side
    devs = 2 * chips
    cols = made.shape[2]
    listed = gat.shape[1]
    half = listed // 2
    me = lax.axis_index('vocab')
    core = lax.rem(me, 2)
    chip = me // 2
    x, y = lax.rem(chip, side), chip // side

    def dev(a, b, c):
        px = lax.rem(x + a * (1 - c) + b * c, side)
        py = lax.rem(y + a * c + b * (1 - c), side)
        return (py * side + px) * 2 + c

    barrier = pltpu.get_barrier_semaphore()

    def greet(i, _):
        pl.semaphore_signal(barrier, inc=1, device_id={'vocab': lax.rem(me + i, devs)}, device_id_type=pl.DeviceIdType.MESH)
        return 0

    def turn(i):
        return lax.rem(chip + 1 + i, chips)

    def head_copy(q):
        return pltpu.make_async_copy(head_hbm.at[:, pl.ds(pl.multiple_of(q * 2 * cols, 2 * cols), 2 * cols)], head.at[q], head_sem.at[q])

    def head_start(i, _):
        head_copy(turn(i)).start()
        return 0

    lax.fori_loop(1, devs, greet, 0)
    lax.fori_loop(0, EARLY, head_start, 0)
    hid_copy = pltpu.make_async_copy(hid_hbm, hid, hid_sem)

    prepare(me, head.shape[1], cap, ids_ref, valid_ref, code_ref, pos_ref, pick)
    lax.fori_loop(EARLY, chips, head_start, 0)

    def make(i):
        q = turn(i)
        head_copy(q).wait()
        rows = jnp.dot(pick[...], head[q], preferred_element_type=F32).astype(BF16)
        made[2 * q] = rows[:, :cols]
        made[2 * q + 1] = rows[:, cols:]

    def give(d):
        return pltpu.make_async_remote_copy(
            src_ref=made.at[d], dst_ref=got.at[me], send_sem=made_sem.at[d], recv_sem=got_sem.at[me],
            device_id={'vocab': d}, device_id_type=pl.DeviceIdType.MESH)

    def give_chip(i):
        q = turn(i)
        give(2 * q).start()
        give(2 * q + 1).start()

    def make_give(i, _):
        make(i)

        @pl.when(i == lead)
        def _():
            pl.semaphore_wait(barrier, devs - 1)

        @pl.when(i >= lead)
        def _():
            give_chip(i - lead)

        return 0

    def give_only(i, _):
        give_chip(i)
        return 0

    lax.fori_loop(0, chips, make_give, 0)
    hid_copy.start()
    lax.fori_loop(chips - lead, chips - 1, give_only, 0)
    mate = chip * 2 + 1 - core
    compact(code_ref, pos_ref, slot_ref)
    part[...] = jnp.zeros_like(part)
    got[me] = made[me]
    give(mate).start()

    def got_wait(r):
        pltpu.make_async_remote_copy(
            src_ref=made.at[r], dst_ref=got.at[r], send_sem=made_sem.at[r], recv_sem=got_sem.at[r],
            device_id={'vocab': r}, device_id_type=pl.DeviceIdType.MESH).wait_recv()

    step = min(2 * cap, 256)
    band = math.gcd(256, listed)
    wide = band if compact_code else listed

    def place(q):
        base = q * (2 * cap)
        pair = got[pl.ds(2 * q, 2)].reshape(2 * cap, cols)
        for k in range(2 * cap // step):
            slots = pair[k * step:(k + 1) * step]
            for m in range(listed // band):
                where = slot_ref[pl.ds(m * band, band), :] - base - k * step
                hot = []
                for c in range(0, step, 128):
                    w = min(128, step - c)
                    ids = lax.broadcasted_iota(I32, (band, 128), 1) + c
                    hot.append(jnp.where(where == ids, 1.0, 0.0).astype(BF16)[:, :w])
                hot = jnp.concatenate(hot, axis=1) if len(hot) > 1 else hot[0]
                part[pl.ds(m * band, band), :] += jnp.dot(hot, slots, preferred_element_type=F32)

    def place_step(i, _):
        middle = chips // 2
        q = lax.rem(chip + chips - i - (i < middle).astype(I32) + (i == middle).astype(I32) * middle, chips)

        @pl.when(i != middle)
        def _():
            got_wait(2 * q)
            got_wait(2 * q + 1)

        @pl.when(i == middle)
        def _():
            got_wait(mate)

        place(q)
        return 0

    lax.fori_loop(0, chips, place_step, 0)
    gat[me] = part[...].astype(BF16)
    hid_copy.wait()
    acc[...] = jnp.zeros_like(acc)

    def piece(ref, d, h):
        return ref.at[d, pl.ds(h * half, half), :]

    def slot(a, b, h):
        return ((a % side) * side + (b % side)) * 2 + h

    sent = []

    def ring_copy(k, a, b, h, da, db):
        d = dev(a % side, b % side, core)
        to = dev(da % side, db % side, core)
        return pltpu.make_async_remote_copy(
            src_ref=piece(gat, d, h), dst_ref=piece(gat, d, h), send_sem=ring_send.at[k],
            recv_sem=ring_recv.at[slot(a - da, b - db, h)], device_id={'vocab': to}, device_id_type=pl.DeviceIdType.MESH)

    def ring(*at):
        ring_copy(len(sent), *at).start()
        sent.append(at)

    def pair_copy(a, b, h, c):
        d = dev(a % side, b % side, c)
        return pltpu.make_async_remote_copy(
            src_ref=piece(gat, d, h), dst_ref=piece(gat, d, h), send_sem=pair_send.at[slot(a, b, h)],
            recv_sem=pair_recv.at[slot(a, b, h)], device_id={'vocab': mate}, device_id_type=pl.DeviceIdType.MESH)

    def arrive(a, b, h):
        d = dev(a % side, b % side, core)
        pltpu.make_async_remote_copy(
            src_ref=piece(gat, d, h), dst_ref=piece(gat, d, h), send_sem=ring_send.at[0],
            recv_sem=ring_recv.at[slot(a, b, h)], device_id={'vocab': mate}, device_id_type=pl.DeviceIdType.MESH).wait_recv()

    def ready(a, b):
        for h in range(2):
            pair_copy(a, b, h, 1 - core).wait_recv()

    def add(slices):
        lhs = jnp.concatenate([hid[:, pl.ds(pl.multiple_of(d * cols, cols), cols)] for d in slices], axis=1)

        def columns(m, _):
            at = pl.ds(pl.multiple_of(m * wide, 128), wide)
            rhs = jnp.concatenate([gat[d, at, :] for d in slices], axis=1)
            acc[:, at] += lax.dot_general(lhs, rhs, (((1,), (1,)), ((), ())), preferred_element_type=F32)
            return 0

        lax.fori_loop(0, listed // wide, columns, 0)

    far = side // 2

    def take(a, b, h):
        if (a, b) != (0, 0):
            arrive(a, b, h)
        if b == 0:
            if a == 0:
                order = (-1, 1) if h == 0 else (1, -1)
                for s in order:
                    ring(a, b, h, s, 0)
            elif a == 1 and h == 0:
                ring(a, b, h, -1, 0)
            elif a == -1 and h == 1:
                ring(a, b, h, 1, 0)
            for s in (-1, 1):
                ring(a, b, h, 0, s)
        elif b == 1 and h == 0:
            ring(a, b, h, 0, -1)
        elif b == -1 and h == 1:
            ring(a, b, h, 0, 1)
        pair_copy(a, b, h, core).start()

    for s, h in ((-1, 0), (1, 1)):
        ring(0, 0, h, s, 0)
        ring(0, 0, h, 0, s)
    for h in range(2):
        pair_copy(0, 0, h, core).start()
    for s, h in ((-1, 1), (1, 0)):
        ring(0, 0, h, s, 0)
        ring(0, 0, h, 0, s)

    phases = [
        ([(1, 0, 0), (-1, 0, 1), (0, 1, 0), (0, -1, 1)], (0, 0)),
        ([(1, 0, 1), (-1, 0, 0), (0, 1, 1), (0, -1, 0)], (1, 0)),
        ([], (-1, 0)),
        ([(far, 0, 0), (far, 0, 1)], (0, 1)),
        ([(1, 1, 0), (-1, -1, 1), (1, -1, 0), (-1, 1, 1)], (0, -1)),
        ([(1, 1, 1), (1, -1, 1), (-1, -1, 0), (-1, 1, 0)], (far, 0)),
        ([(0, far, 0), (0, far, 1)], (1, 1)),
        ([], (-1, -1)),
        ([(far, 1, 0), (far, -1, 1)], (-1, 1)),
        ([], (1, -1)),
        ([(far, 1, 1), (far, -1, 0)], (0, far)),
        ([(1, far, 0), (1, far, 1)], (far, 1)),
        ([], (far, -1)),
        ([(-1, far, 0), (-1, far, 1)], (1, far)),
        ([], (-1, far)),
        ([(far, far, 0), (far, far, 1)], (far, far)),
    ]

    def phase(p, _):
        a, b = 0, 0
        for k, (takes, place) in enumerate(phases):
            @pl.when(p == k)
            def _():
                for t in takes:
                    take(*t)
                ready(*place)

            here = (p == k).astype(I32)
            a, b = a + here * (place[0] % side), b + here * (place[1] % side)
        add([dev(a, b, core), dev(a, b, 1 - core)])
        return 0

    lax.fori_loop(0, len(phases), phase, 0)

    for k, at in enumerate(sent):
        ring_copy(k, *at).wait_send()
    for a in range(side):
        for b in range(side):
            for h in range(2):
                pair_copy(a, b, h, core).wait_send()

    def given(i, _):
        give(lax.rem(me + i, devs)).wait_send()
        return 0

    lax.fori_loop(1, devs, given, 0)


def gather_scores(shards, listed, cap, compact_code, collective_id, hidden, w_head, ids, valid):
    rows, depth = hidden.shape
    n = ids.shape[0] * ids.shape[1]
    vocab_local = w_head.shape[0]
    cols = depth // shards
    side = math.isqrt(shards // 2)
    vmem = pl.BlockSpec(memory_space=pltpu.VMEM)
    hbm = pl.BlockSpec(memory_space=pl.ANY)
    dma = pltpu.SemaphoreType.DMA
    limit = 2 * (rows * depth + vocab_local * depth + cap * (vocab_local + 2 * depth) + listed * depth + 4 * (n + listed) * cols) + 10 * 1024 * 1024
    return pl.pallas_call(
        functools.partial(gather_kernel, side, cap, LEAD, compact_code),
        out_shape=jax.ShapeDtypeStruct((rows, listed), F32),
        in_specs=[hbm, hbm, vmem, vmem],
        out_specs=vmem,
        scratch_shapes=[
            pltpu.VMEM((rows, depth), BF16),
            pltpu.VMEM((shards // 2, vocab_local, 2 * cols), BF16),
            pltpu.VMEM((n, 128), I32),
            pltpu.VMEM((n, 128), I32),
            pltpu.VMEM((listed, 128), I32),
            pltpu.VMEM((cap, vocab_local), BF16),
            pltpu.VMEM((shards, cap, cols), BF16),
            pltpu.VMEM((shards, cap, cols), BF16),
            pltpu.VMEM((listed, cols), F32),
            pltpu.VMEM((shards, listed, cols), BF16),
            dma, dma((shards // 2,)), dma((shards,)), dma((shards,)),
            dma((30,)), dma((shards,)), dma((shards,)), dma((shards,)),
        ],
        compiler_params=pltpu.CompilerParams(collective_id=collective_id, has_side_effects=True, vmem_limit_bytes=limit),
        name=f'gather_scores_{listed}_{cap}',
    )(hidden, w_head, ids, valid)


def finish_kernel(band, score_ref, valid_ref, target_ref, probs_ref, logp_ref, cols_ref, place_ref, local_ref):
    rows, n = probs_ref.shape
    last = score_ref.shape[1] - 128
    chunks = n // 128

    @pl.when(pl.program_id(0) == 0)
    def _():
        flags = valid_ref[...].astype(F32)
        upper = (lax.broadcasted_iota(I32, (128, 128), 0) < lane_ids(128)).astype(F32).astype(BF16)
        inner = jnp.dot(flags.astype(BF16), upper, preferred_element_type=F32)
        totals = jnp.broadcast_to(jnp.sum(flags, axis=1, keepdims=True), (chunks, 128))
        above = (lax.broadcasted_iota(I32, (chunks, chunks), 0) > lax.broadcasted_iota(I32, (chunks, chunks), 1)).astype(F32)
        base = jnp.dot(above.astype(BF16), totals.astype(BF16), preferred_element_type=F32).astype(I32)
        local_ref[...] = (inner.astype(I32) + base) & 127
        for c in range(chunks):
            place_ref[c] = base[c, 0]

    first = pl.program_id(0) * rows
    cols_ref[...] = column(target_ref[0].astype(F32))[:rows]

    def some(r, _):
        at = pl.ds(pl.multiple_of(r * band, band), band)
        from_rows = pl.ds(pl.multiple_of(first + r * band, band), band)
        target = cols_ref[at, :].astype(I32)
        top = jnp.full((band, 128), -jnp.inf, F32)
        picked = jnp.zeros((band, 128), F32)
        for c in range(chunks):
            begin = place_ref[c]
            whole = begin & -128
            lower = score_ref[from_rows, pl.ds(pl.multiple_of(jnp.minimum(whole, last), 128), 128)]
            upper = score_ref[from_rows, pl.ds(pl.multiple_of(jnp.minimum(whole + 128, last), 128), 128)]
            window = jnp.where(lane_ids(band) >= begin - whole, lower, upper)
            local = jnp.broadcast_to(local_ref[c:c + 1, :], (band, 128))
            part = jnp.take_along_axis(window, local, axis=1, mode='promise_in_bounds')
            part = jnp.where(valid_ref[c:c + 1, :] > 0, part, -jnp.inf)
            probs_ref[at, c * 128:(c + 1) * 128] = part
            top = jnp.maximum(top, part)
            picked += jnp.where(target == lane_ids(band) + c * 128, part, 0.0)
        top = jnp.max(top, axis=1, keepdims=True)
        total = jnp.zeros((band, 128), F32)
        for c in range(chunks):
            terms = jnp.exp((probs_ref[at, c * 128:(c + 1) * 128] - top) * INV_TEMP)
            probs_ref[at, c * 128:(c + 1) * 128] = terms
            total += terms
        total = jnp.sum(total, axis=1, keepdims=True)
        probs_ref[at, :] = probs_ref[at, :] * (1.0 / total)
        logp = (jnp.sum(picked, axis=1, keepdims=True) - top) * INV_TEMP - jnp.log(total)
        cols_ref[at, :] = jnp.broadcast_to(logp, (band, 128))
        return 0

    lax.fori_loop(0, rows // band, some, 0)
    logp_ref[0] = jnp.transpose(cols_ref[...])[:1]


def finish(scores, valid, target_pos, band):
    rows = scores.shape[0]
    n = valid.shape[0] * valid.shape[1]
    block = min(128, rows)
    band = min(band, block)
    probs, logp = pl.pallas_call(
        functools.partial(finish_kernel, band),
        grid=(rows // block,),
        out_shape=(jax.ShapeDtypeStruct((rows, n), F32), jax.ShapeDtypeStruct((rows // block, 1, block), F32)),
        in_specs=[pl.BlockSpec(memory_space=pltpu.VMEM), pl.BlockSpec(valid.shape, lambda i: (0, 0)),
                  pl.BlockSpec((1, 1, block), lambda i: (i, 0, 0))],
        out_specs=(pl.BlockSpec((block, n), lambda i: (i, 0)), pl.BlockSpec((1, 1, block), lambda i: (i, 0, 0))),
        scratch_shapes=[pltpu.VMEM((block, 128), F32), pltpu.SMEM((n // 128,), I32), pltpu.VMEM((n // 128, 128), I32)],
        compiler_params=pltpu.CompilerParams(dimension_semantics=('arbitrary',), vmem_limit_bytes=16 * 1024 * 1024),
        name='finish',
    )(scores, valid, target_pos.reshape(rows // block, 1, block))
    return probs, logp.reshape(rows)


def choose_kernel(shards, vocab_local, fits, ids_ref, valid_ref, choice_ref):
    owner = jnp.where(valid_ref[...] > 0, power_div(ids_ref[...], vocab_local), -1)
    counts = [jnp.sum((owner == r).astype(F32), axis=0, keepdims=True) for r in range(shards)]
    counts = jnp.sum(jnp.concatenate(counts, axis=0), axis=1, keepdims=True)
    most, every = jnp.max(counts), jnp.sum(counts)
    choice = jnp.int32(0)
    for size, cap in fits:
        choice += jnp.where((every <= float(size)) & (most <= float(cap)), jnp.int32(0), jnp.int32(1))
    choice_ref[0] = choice


def choose(shards, vocab_local, fits, ids, valid):
    return pl.pallas_call(
        functools.partial(choose_kernel, shards, vocab_local, fits),
        out_shape=jax.ShapeDtypeStruct((1,), I32),
        in_specs=[pl.BlockSpec(memory_space=pltpu.VMEM)] * 2,
        out_specs=pl.BlockSpec(memory_space=pltpu.SMEM),
        compiler_params=pltpu.CompilerParams(vmem_limit_bytes=1024 * 1024),
        name='choose',
    )(ids, valid)[0]


def plans(n, shards, vocab_local):
    mean = 2 * n // shards
    sizes = [-(-n * i // 1024) * 128 for i in SIZES]
    caps = [min(mean, -(-(mean * size // n + mean // SPARE) // 8) * 8) for size in sizes]
    return list(zip(sizes, caps)) + [(n, vocab_local)]


def solution(mesh):
    shards = mesh.shape['vocab']

    def device_step(hidden, w_head, allowed_ids, allowed_valid, target_pos):
        vocab_local = w_head.shape[0]
        n = allowed_ids.shape[0]
        runs = []
        for i, (size, cap) in enumerate(plans(n, shards, vocab_local)):
            last = cap == vocab_local

            def run(hidden, w_head, ids, valid, target, size=size, cap=cap, last=last, i=i):
                return finish(gather_scores(shards, size, cap, last, i, hidden, w_head, ids, valid), valid, target, 32 if last else 128)

            runs.append(run)
        ids, valid = allowed_ids.reshape(n // 128, 128), allowed_valid.reshape(n // 128, 128)
        choice = choose(shards, vocab_local, plans(n, shards, vocab_local)[:-1], ids, valid)
        return lax.switch(choice, runs, hidden, w_head, ids, valid, target_pos)

    row_spec = P(('rep', 'vocab'))
    mat_spec = P(('rep', 'vocab'), None)
    return jax.shard_map(device_step, mesh=mesh, in_specs=(mat_spec, P('vocab', None), P('rep'), P('rep'), row_spec), out_specs=(mat_spec, row_spec), check_vma=False)
```

```python
import functools
import math

import jax
import jax.numpy as jnp
from jax import lax
from jax.experimental import pallas as pl
from jax.experimental.pallas import tpu as pltpu
from jax.sharding import PartitionSpec as P

INV_TEMP = 1.25
SIZES = (5, 6, 7, 8)
SPARE = 16
EARLY = 2
LEAD = 2
F32, BF16, I32 = jnp.float32, jnp.bfloat16, jnp.int32


def column(row):
    return jnp.transpose(jnp.broadcast_to(row, (128, 128)))


def lane_ids(rows):
    return lax.broadcasted_iota(I32, (rows, 128), 1)


def power_div(value, by):
    return value >> (by.bit_length() - 1) if by & (by - 1) == 0 else value // by


def prepare(me, vocab_local, cap, ids_ref, valid_ref, code_ref, pos_ref, pick):
    lanes = lane_ids(128)
    below = (lax.broadcasted_iota(I32, (128, 128), 0) > lanes).astype(F32).astype(BF16)
    before = jnp.zeros((1, 128), F32)
    mine = [jnp.zeros((1, 128), F32) for _ in range(-(-cap // 128))]
    for b in range(ids_ref.shape[0]):
        ids = jnp.where(valid_ref[b:b + 1, :] > 0, ids_ref[b:b + 1, :], -1)
        ids = column(ids.astype(F32)).astype(I32)
        valid = ids >= 0
        owner = jnp.where(valid, power_div(ids, vocab_local), -1)
        own = (owner == lanes).astype(F32)
        hot = jnp.where((lanes == 127) & valid, 1.0, own)
        number = jnp.dot(below, hot.astype(BF16), preferred_element_type=F32) + before
        before = before + jnp.sum(hot, axis=0, keepdims=True)
        pos = jnp.sum(jnp.where(lanes == 127, number, 0.0), axis=1, keepdims=True).astype(I32)
        number = jnp.sum(own * number, axis=1, keepdims=True).astype(I32)
        code = jnp.where(valid, owner * cap + number, -1)
        code_ref[b * 128:(b + 1) * 128, :] = code
        pos_ref[b * 128:(b + 1) * 128, :] = jnp.where(valid, pos, -1)
        local = (ids - me * vocab_local + 1).astype(F32)
        for c in range(len(mine)):
            mine[c] += jnp.sum(jnp.where(code == lanes + (me * cap + c * 128), local, 0.0), axis=0, keepdims=True)
    for c in range(len(mine)):
        rows = min(128, cap - c * 128)
        local = (column(mine[c]) - 1.0).astype(I32)[:rows]
        for k in range(0, vocab_local, 128):
            pick[c * 128:c * 128 + rows, k:k + 128] = (local == lane_ids(rows) + k).astype(F32).astype(BF16)


def compact(code_ref, pos_ref, slot_ref):
    def block(b, total, k):
        at = pl.ds(pl.multiple_of(b * 128, 128), 128)
        here = jnp.where(pos_ref[at, :] == lane_ids(128) + k * 128, code_ref[at, :] + 1, 0)
        return total + jnp.sum(here.reshape(16, 8, 128), axis=0)

    for k in range(slot_ref.shape[0] // 128):
        total = lax.fori_loop(k, code_ref.shape[0] // 128, functools.partial(block, k=k), jnp.zeros((8, 128), I32))
        row = jnp.sum(total.astype(F32), axis=0, keepdims=True) - 1.0
        slot_ref[k * 128:(k + 1) * 128, :] = column(row).astype(I32)


def gather_kernel(side, cap, lead, compact_code, hid_hbm, head_hbm, ids_ref, valid_ref, acc,
                  hid, head, code_ref, pos_ref, slot_ref, pick, made, got, part, gat,
                  hid_sem, head_sem, made_sem, got_sem, ring_send, ring_recv, pair_send, pair_recv):
    chips = side * side
    devs = 2 * chips
    cols = made.shape[2]
    listed = gat.shape[1]
    half = listed // 2
    me = lax.axis_index('vocab')
    core = lax.rem(me, 2)
    chip = me // 2
    x, y = lax.rem(chip, side), chip // side

    def dev(a, b, c):
        px = lax.rem(x + a * (1 - c) + b * c, side)
        py = lax.rem(y + a * c + b * (1 - c), side)
        return (py * side + px) * 2 + c

    barrier = pltpu.get_barrier_semaphore()

    def greet(i, _):
        pl.semaphore_signal(barrier, inc=1, device_id={'vocab': lax.rem(me + i, devs)}, device_id_type=pl.DeviceIdType.MESH)
        return 0

    def turn(i):
        return lax.rem(chip + 1 + i, chips)

    def head_copy(q):
        return pltpu.make_async_copy(head_hbm.at[:, pl.ds(pl.multiple_of(q * 2 * cols, 2 * cols), 2 * cols)], head.at[q], head_sem.at[q])

    def head_start(i, _):
        head_copy(turn(i)).start()
        return 0

    lax.fori_loop(1, devs, greet, 0)
    lax.fori_loop(0, EARLY, head_start, 0)
    hid_copy = pltpu.make_async_copy(hid_hbm, hid, hid_sem)

    prepare(me, head.shape[1], cap, ids_ref, valid_ref, code_ref, pos_ref, pick)
    lax.fori_loop(EARLY, chips, head_start, 0)

    def make(i):
        q = turn(i)
        head_copy(q).wait()
        rows = jnp.dot(pick[...], head[q], preferred_element_type=F32).astype(BF16)
        made[2 * q] = rows[:, :cols]
        made[2 * q + 1] = rows[:, cols:]

    def give(d):
        return pltpu.make_async_remote_copy(
            src_ref=made.at[d], dst_ref=got.at[me], send_sem=made_sem.at[d], recv_sem=got_sem.at[me],
            device_id={'vocab': d}, device_id_type=pl.DeviceIdType.MESH)

    def give_chip(i):
        q = turn(i)
        give(2 * q).start()
        give(2 * q + 1).start()

    def make_give(i, _):
        make(i)

        @pl.when(i == lead)
        def _():
            pl.semaphore_wait(barrier, devs - 1)

        @pl.when(i >= lead)
        def _():
            give_chip(i - lead)

        return 0

    def give_only(i, _):
        give_chip(i)
        return 0

    lax.fori_loop(0, chips, make_give, 0)
    hid_copy.start()
    lax.fori_loop(chips - lead, chips - 1, give_only, 0)
    mate = chip * 2 + 1 - core
    compact(code_ref, pos_ref, slot_ref)
    part[...] = jnp.zeros_like(part)
    acc[...] = jnp.zeros_like(acc)
    got[me] = made[me]
    give(mate).start()

    def got_wait(r):
        pltpu.make_async_remote_copy(
            src_ref=made.at[r], dst_ref=got.at[r], send_sem=made_sem.at[r], recv_sem=got_sem.at[r],
            device_id={'vocab': r}, device_id_type=pl.DeviceIdType.MESH).wait_recv()

    step = min(2 * cap, 256)
    band = math.gcd(256, listed)
    wide = band if compact_code else listed

    def place(q):
        base = q * (2 * cap)
        pair = got[pl.ds(2 * q, 2)].reshape(2 * cap, cols)
        for k in range(2 * cap // step):
            slots = pair[k * step:(k + 1) * step]
            for m in range(listed // band):
                where = slot_ref[pl.ds(m * band, band), :] - base - k * step
                hot = []
                for c in range(0, step, 128):
                    w = min(128, step - c)
                    ids = lax.broadcasted_iota(I32, (band, 128), 1) + c
                    hot.append(jnp.where(where == ids, 1.0, 0.0).astype(BF16)[:, :w])
                hot = jnp.concatenate(hot, axis=1) if len(hot) > 1 else hot[0]
                part[pl.ds(m * band, band), :] += jnp.dot(hot, slots, preferred_element_type=F32)

    def place_step(i, _):
        middle = chips // 2
        q = lax.rem(chip + chips - i - (i < middle).astype(I32) + (i == middle).astype(I32) * middle, chips)

        @pl.when(i != middle)
        def _():
            got_wait(2 * q)
            got_wait(2 * q + 1)

        @pl.when(i == middle)
        def _():
            got_wait(mate)

        place(q)
        return 0

    lax.fori_loop(0, chips, place_step, 0)
    gat[me] = part[...].astype(BF16)

    def piece(ref, d, h):
        return ref.at[d, pl.ds(h * half, half), :]

    def slot(a, b, h):
        return ((a % side) * side + (b % side)) * 2 + h

    sent = []

    def ring_copy(k, a, b, h, da, db):
        d = dev(a % side, b % side, core)
        to = dev(da % side, db % side, core)
        return pltpu.make_async_remote_copy(
            src_ref=piece(gat, d, h), dst_ref=piece(gat, d, h), send_sem=ring_send.at[k],
            recv_sem=ring_recv.at[slot(a - da, b - db, h)], device_id={'vocab': to}, device_id_type=pl.DeviceIdType.MESH)

    def ring(*at):
        ring_copy(len(sent), *at).start()
        sent.append(at)

    def pair_copy(a, b, h, c):
        d = dev(a % side, b % side, c)
        return pltpu.make_async_remote_copy(
            src_ref=piece(gat, d, h), dst_ref=piece(gat, d, h), send_sem=pair_send.at[slot(a, b, h)],
            recv_sem=pair_recv.at[slot(a, b, h)], device_id={'vocab': mate}, device_id_type=pl.DeviceIdType.MESH)

    def arrive(a, b, h):
        d = dev(a % side, b % side, core)
        pltpu.make_async_remote_copy(
            src_ref=piece(gat, d, h), dst_ref=piece(gat, d, h), send_sem=ring_send.at[0],
            recv_sem=ring_recv.at[slot(a, b, h)], device_id={'vocab': mate}, device_id_type=pl.DeviceIdType.MESH).wait_recv()

    def ready(a, b):
        for h in range(2):
            pair_copy(a, b, h, 1 - core).wait_recv()

    def add(slices):
        lhs = jnp.concatenate([hid[:, pl.ds(pl.multiple_of(d * cols, cols), cols)] for d in slices], axis=1)

        def columns(m, _):
            at = pl.ds(pl.multiple_of(m * wide, 128), wide)
            rhs = jnp.concatenate([gat[d, at, :] for d in slices], axis=1)
            acc[:, at] += lax.dot_general(lhs, rhs, (((1,), (1,)), ((), ())), preferred_element_type=F32)
            return 0

        lax.fori_loop(0, listed // wide, columns, 0)

    far = side // 2

    def take(a, b, h):
        if (a, b) != (0, 0):
            arrive(a, b, h)
        if b == 0:
            if a == 0:
                order = (-1, 1) if h == 0 else (1, -1)
                for s in order:
                    ring(a, b, h, s, 0)
            elif a == 1 and h == 0:
                ring(a, b, h, -1, 0)
            elif a == -1 and h == 1:
                ring(a, b, h, 1, 0)
            for s in (-1, 1):
                ring(a, b, h, 0, s)
        elif b == 1 and h == 0:
            ring(a, b, h, 0, -1)
        elif b == -1 and h == 1:
            ring(a, b, h, 0, 1)
        pair_copy(a, b, h, core).start()

    for s, h in ((-1, 0), (1, 1)):
        ring(0, 0, h, s, 0)
        ring(0, 0, h, 0, s)
    for h in range(2):
        pair_copy(0, 0, h, core).start()
    for s, h in ((-1, 1), (1, 0)):
        ring(0, 0, h, s, 0)
        ring(0, 0, h, 0, s)

    phases = [
        ([(1, 0, 0), (-1, 0, 1), (0, 1, 0), (0, -1, 1)], (0, 0)),
        ([(1, 0, 1), (-1, 0, 0), (0, 1, 1), (0, -1, 0)], (1, 0)),
        ([], (-1, 0)),
        ([(far, 0, 0), (far, 0, 1)], (0, 1)),
        ([(1, 1, 0), (-1, -1, 1), (1, -1, 0), (-1, 1, 1)], (0, -1)),
        ([(1, 1, 1), (1, -1, 1), (-1, -1, 0), (-1, 1, 0)], (far, 0)),
        ([(0, far, 0), (0, far, 1)], (1, 1)),
        ([], (-1, -1)),
        ([(far, 1, 0), (far, -1, 1)], (-1, 1)),
        ([], (1, -1)),
        ([(far, 1, 1), (far, -1, 0)], (0, far)),
        ([(1, far, 0), (1, far, 1)], (far, 1)),
        ([], (far, -1)),
        ([(-1, far, 0), (-1, far, 1)], (1, far)),
        ([], (-1, far)),
        ([(far, far, 0), (far, far, 1)], (far, far)),
    ]

    def phase(p, _):
        a, b = 0, 0
        for k, (takes, place) in enumerate(phases):
            @pl.when(p == k)
            def _():
                for t in takes:
                    take(*t)
                ready(*place)

            here = (p == k).astype(I32)
            a, b = a + here * (place[0] % side), b + here * (place[1] % side)
        add([dev(a, b, core), dev(a, b, 1 - core)])
        return 0

    hid_copy.wait()
    lax.fori_loop(0, len(phases), phase, 0)

    for k, at in enumerate(sent):
        ring_copy(k, *at).wait_send()
    for a in range(side):
        for b in range(side):
            for h in range(2):
                pair_copy(a, b, h, core).wait_send()

    def given(i, _):
        give(lax.rem(me + i, devs)).wait_send()
        return 0

    lax.fori_loop(1, devs, given, 0)


def gather_scores(shards, listed, cap, compact_code, collective_id, hidden, w_head, ids, valid):
    rows, depth = hidden.shape
    n = ids.shape[0] * ids.shape[1]
    vocab_local = w_head.shape[0]
    cols = depth // shards
    side = math.isqrt(shards // 2)
    vmem = pl.BlockSpec(memory_space=pltpu.VMEM)
    hbm = pl.BlockSpec(memory_space=pl.ANY)
    dma = pltpu.SemaphoreType.DMA
    limit = 2 * (rows * depth + vocab_local * depth + cap * (vocab_local + 2 * depth) + listed * depth + 4 * (n + listed) * cols) + 10 * 1024 * 1024
    return pl.pallas_call(
        functools.partial(gather_kernel, side, cap, LEAD, compact_code),
        out_shape=jax.ShapeDtypeStruct((rows, listed), F32),
        in_specs=[hbm, hbm, vmem, vmem],
        out_specs=vmem,
        scratch_shapes=[
            pltpu.VMEM((rows, depth), BF16),
            pltpu.VMEM((shards // 2, vocab_local, 2 * cols), BF16),
            pltpu.VMEM((n, 128), I32),
            pltpu.VMEM((n, 128), I32),
            pltpu.VMEM((listed, 128), I32),
            pltpu.VMEM((cap, vocab_local), BF16),
            pltpu.VMEM((shards, cap, cols), BF16),
            pltpu.VMEM((shards, cap, cols), BF16),
            pltpu.VMEM((listed, cols), F32),
            pltpu.VMEM((shards, listed, cols), BF16),
            dma, dma((shards // 2,)), dma((shards,)), dma((shards,)),
            dma((30,)), dma((shards,)), dma((shards,)), dma((shards,)),
        ],
        compiler_params=pltpu.CompilerParams(collective_id=collective_id, has_side_effects=True, vmem_limit_bytes=limit),
        name=f'gather_scores_{listed}_{cap}',
    )(hidden, w_head, ids, valid)


def finish_kernel(band, score_ref, valid_ref, target_ref, probs_ref, logp_ref, cols_ref, place_ref, local_ref):
    rows, n = probs_ref.shape
    last = score_ref.shape[1] - 128
    chunks = n // 128

    @pl.when(pl.program_id(0) == 0)
    def _():
        flags = valid_ref[...].astype(F32)
        upper = (lax.broadcasted_iota(I32, (128, 128), 0) < lane_ids(128)).astype(F32).astype(BF16)
        inner = jnp.dot(flags.astype(BF16), upper, preferred_element_type=F32)
        totals = jnp.broadcast_to(jnp.sum(flags, axis=1, keepdims=True), (chunks, 128))
        above = (lax.broadcasted_iota(I32, (chunks, chunks), 0) > lax.broadcasted_iota(I32, (chunks, chunks), 1)).astype(F32)
        base = jnp.dot(above.astype(BF16), totals.astype(BF16), preferred_element_type=F32).astype(I32)
        local_ref[...] = (inner.astype(I32) + base) & 127
        for c in range(chunks):
            place_ref[c] = base[c, 0]

    first = pl.program_id(0) * rows
    cols_ref[...] = column(target_ref[0].astype(F32))[:rows]

    def some(r, _):
        at = pl.ds(pl.multiple_of(r * band, band), band)
        from_rows = pl.ds(pl.multiple_of(first + r * band, band), band)
        target = cols_ref[at, :].astype(I32)
        top = jnp.full((band, 128), -jnp.inf, F32)
        picked = jnp.zeros((band, 128), F32)
        for c in range(chunks):
            begin = place_ref[c]
            whole = begin & -128
            lower = score_ref[from_rows, pl.ds(pl.multiple_of(jnp.minimum(whole, last), 128), 128)]
            upper = score_ref[from_rows, pl.ds(pl.multiple_of(jnp.minimum(whole + 128, last), 128), 128)]
            window = jnp.where(lane_ids(band) >= begin - whole, lower, upper)
            local = jnp.broadcast_to(local_ref[c:c + 1, :], (band, 128))
            part = jnp.take_along_axis(window, local, axis=1, mode='promise_in_bounds')
            part = jnp.where(valid_ref[c:c + 1, :] > 0, part, -jnp.inf)
            probs_ref[at, c * 128:(c + 1) * 128] = part
            top = jnp.maximum(top, part)
            picked += jnp.where(target == lane_ids(band) + c * 128, part, 0.0)
        top = jnp.max(top, axis=1, keepdims=True)
        total = jnp.zeros((band, 128), F32)
        for c in range(chunks):
            terms = jnp.exp((probs_ref[at, c * 128:(c + 1) * 128] - top) * INV_TEMP)
            probs_ref[at, c * 128:(c + 1) * 128] = terms
            total += terms
        total = jnp.sum(total, axis=1, keepdims=True)
        probs_ref[at, :] = probs_ref[at, :] * (1.0 / total)
        logp = (jnp.sum(picked, axis=1, keepdims=True) - top) * INV_TEMP - jnp.log(total)
        cols_ref[at, :] = jnp.broadcast_to(logp, (band, 128))
        return 0

    lax.fori_loop(0, rows // band, some, 0)
    logp_ref[0] = jnp.transpose(cols_ref[...])[:1]


def finish(scores, valid, target_pos, band):
    rows = scores.shape[0]
    n = valid.shape[0] * valid.shape[1]
    block = min(128, rows)
    band = min(band, block)
    probs, logp = pl.pallas_call(
        functools.partial(finish_kernel, band),
        grid=(rows // block,),
        out_shape=(jax.ShapeDtypeStruct((rows, n), F32), jax.ShapeDtypeStruct((rows // block, 1, block), F32)),
        in_specs=[pl.BlockSpec(memory_space=pltpu.VMEM), pl.BlockSpec(valid.shape, lambda i: (0, 0)),
                  pl.BlockSpec((1, 1, block), lambda i: (i, 0, 0))],
        out_specs=(pl.BlockSpec((block, n), lambda i: (i, 0)), pl.BlockSpec((1, 1, block), lambda i: (i, 0, 0))),
        scratch_shapes=[pltpu.VMEM((block, 128), F32), pltpu.SMEM((n // 128,), I32), pltpu.VMEM((n // 128, 128), I32)],
        compiler_params=pltpu.CompilerParams(dimension_semantics=('arbitrary',), vmem_limit_bytes=16 * 1024 * 1024),
        name='finish',
    )(scores, valid, target_pos.reshape(rows // block, 1, block))
    return probs, logp.reshape(rows)


def choose_kernel(shards, vocab_local, fits, ids_ref, valid_ref, choice_ref):
    owner = jnp.where(valid_ref[...] > 0, power_div(ids_ref[...], vocab_local), -1)
    counts = [jnp.sum((owner == r).astype(F32), axis=0, keepdims=True) for r in range(shards)]
    counts = jnp.sum(jnp.concatenate(counts, axis=0), axis=1, keepdims=True)
    most, every = jnp.max(counts), jnp.sum(counts)
    choice = jnp.int32(0)
    for size, cap in fits:
        choice += jnp.where((every <= float(size)) & (most <= float(cap)), jnp.int32(0), jnp.int32(1))
    choice_ref[0] = choice


def choose(shards, vocab_local, fits, ids, valid):
    return pl.pallas_call(
        functools.partial(choose_kernel, shards, vocab_local, fits),
        out_shape=jax.ShapeDtypeStruct((1,), I32),
        in_specs=[pl.BlockSpec(memory_space=pltpu.VMEM)] * 2,
        out_specs=pl.BlockSpec(memory_space=pltpu.SMEM),
        compiler_params=pltpu.CompilerParams(vmem_limit_bytes=1024 * 1024),
        name='choose',
    )(ids, valid)[0]


def plans(n, shards, vocab_local):
    mean = 2 * n // shards
    sizes = [-(-n * i // 1024) * 128 for i in SIZES]
    caps = [min(mean, -(-(mean * size // n + mean // SPARE) // 8) * 8) for size in sizes]
    return list(zip(sizes, caps)) + [(n, vocab_local)]


def solution(mesh):
    shards = mesh.shape['vocab']

    def device_step(hidden, w_head, allowed_ids, allowed_valid, target_pos):
        vocab_local = w_head.shape[0]
        n = allowed_ids.shape[0]
        runs = []
        for i, (size, cap) in enumerate(plans(n, shards, vocab_local)):
            last = cap == vocab_local

            def run(hidden, w_head, ids, valid, target, size=size, cap=cap, last=last, i=i):
                return finish(gather_scores(shards, size, cap, last, i, hidden, w_head, ids, valid), valid, target, 32 if last else 128)

            runs.append(run)
        ids, valid = allowed_ids.reshape(n // 128, 128), allowed_valid.reshape(n // 128, 128)
        choice = choose(shards, vocab_local, plans(n, shards, vocab_local)[:-1], ids, valid)
        return lax.switch(choice, runs, hidden, w_head, ids, valid, target_pos)

    row_spec = P(('rep', 'vocab'))
    mat_spec = P(('rep', 'vocab'), None)
    return jax.shard_map(device_step, mesh=mesh, in_specs=(mat_spec, P('vocab', None), P('rep'), P('rep'), row_spec), out_specs=(mat_spec, row_spec), check_vma=False)
```
